128 devices in a mesh: lat: 2 (over x_lo), lon: 8 (over z_lo, x_hi, core), lev: 8 (over z_hi, y).
Axes of the slice: x: 4 (x_hi: 2, x_lo: 2; x = x_hi * 2 + x_lo), y: 4, z: 4 (z_hi: 2, z_lo: 2; z = z_hi * 2 + z_lo), core: 2. Of those that a mesh axis runs over, the one named last changes fastest.
Arguments:
- initial_state: float32 [16, 256, 512, 128], P('lat', 'lon', 'lev'), may hold values from 0.2 to 1.8
- scaled_diffusivity: float32 [16, 256, 512, 128], P('lat', 'lon', 'lev'), may hold values from 0.03 to 0.15
- scaled_forcing: float32 [16, 256, 512, 128], P('lat', 'lon', 'lev'), may hold values from -0.2 to 0.2
Outputs:
- cumulative_totals: float32 [16, 256, 512, 128], P('lat', 'lon', 'lev')
- temperature_end: float32 [16, 256, 512, 128], P('lat', 'lon', 'lev')
The draws below stay inside these ranges and needn't reach their ends.
All inputs are finite; a program needn't handle non-finite values.
Results may differ from the reference program's by a relative error of at most 0.00002.
Values sent between devices are 32-bit elements; how exact they have to be, the bound alone decides.
A program may use at most 128 MiB of HBM per device.

```python
import jax
import jax.numpy as jnp
from jax import lax

SECOND_EXTENT = 16
FIRST_EXTENT = 256
THIRD_EXTENT = 512
MEMBER_TALLY = 128
STEPS = 4


def level_of(rng, extent, cuts, smallest, top_value):
    def one(axis_at, shards_of):
        draws = jax.random.uniform(jax.random.fold_in(jax.random.fold_in(rng, 6), axis_at), (shards_of,), jnp.float32, smallest / len(cuts), top_value / len(cuts))
        return jnp.repeat(jnp.exp(draws), extent[axis_at] // shards_of).reshape((-1,) + (1,) * (len(extent) - axis_at - 1))

    level = one(*cuts[0])
    for cut in cuts[1:]:
        level = level * one(*cut)
    return level


def setup_inputs(seed: int = 0) -> dict:
    seeds = jax.random.split(jax.random.key(seed), 4)
    initial_state = jnp.clip(0.2 + 1.5999999 * jax.random.uniform(seeds[0], (SECOND_EXTENT, FIRST_EXTENT, THIRD_EXTENT, MEMBER_TALLY), jnp.float32) ** level_of(seeds[0], (SECOND_EXTENT, FIRST_EXTENT, THIRD_EXTENT, MEMBER_TALLY), ((0, 2), (1, 8), (2, 8)), -0.2, 0.2), 0.2, 1.8)
    scaled_diffusivity = jnp.clip(0.03 + 0.120000007 * jax.random.uniform(seeds[1], (SECOND_EXTENT, FIRST_EXTENT, THIRD_EXTENT, MEMBER_TALLY), jnp.float32) ** level_of(seeds[1], (SECOND_EXTENT, FIRST_EXTENT, THIRD_EXTENT, MEMBER_TALLY), ((0, 2), (1, 8), (2, 8)), -0.2, 0.2), 0.03, 0.15)
    scaled_forcing = jnp.clip(jax.random.uniform(seeds[2], (SECOND_EXTENT, FIRST_EXTENT, THIRD_EXTENT, MEMBER_TALLY), jnp.float32, -0.2, 0.2) * level_of(seeds[2], (SECOND_EXTENT, FIRST_EXTENT, THIRD_EXTENT, MEMBER_TALLY), ((0, 2), (1, 8), (2, 8)), -0.4, 0.0), -0.2, 0.2)
    return dict(initial_state=initial_state, scaled_diffusivity=scaled_diffusivity, scaled_forcing=scaled_forcing)


def strip_edges(values, dims):
    for dim in dims:
        values = lax.slice_in_dim(values, 1, values.shape[dim] - 1, axis=dim)
    return values


def neighbour(values, dim, start, dims):
    others = [other for other in dims if other != dim]
    values = strip_edges(values, others)
    return lax.slice_in_dim(values, start, start + values.shape[dim] - 2, axis=dim)


def explicit_update(haloed_values, scaled_diffusivity, scaled_forcing):
    middle = strip_edges(haloed_values, (0, 1, 2))
    lower = [neighbour(haloed_values, dim, 0, (0, 1, 2)) for dim in (0, 1, 2)]
    upper = [neighbour(haloed_values, dim, 2, (0, 1, 2)) for dim in (0, 1, 2)]
    spread = lower[0] + upper[0] + lower[1] + upper[1] + lower[2] + upper[2] - 6.0 * middle
    return middle + scaled_diffusivity * spread + scaled_forcing


def reference(initial_state, scaled_diffusivity, scaled_forcing):
    for step in range(STEPS):
        initial_state = explicit_update(jnp.pad(initial_state, ((1, 1), (1, 1), (1, 1), (0, 0)), mode="constant"), scaled_diffusivity, scaled_forcing)
    cumulative_totals = jnp.cumsum(initial_state, axis=1) / FIRST_EXTENT
    return cumulative_totals, initial_state
```

```python
import jax
import jax.numpy as jnp
from jax import lax
from jax.experimental import pallas as pl
from jax.experimental.pallas import tpu as pltpu
from jax.sharding import PartitionSpec as P

STEPS = 4
MESH = pl.DeviceIdType.MESH
Q, N, K, M = 8, 32, 64, 128
PAD = 8
TOP = PAD + K
CHUNKS = 8
ROWS = N // CHUNKS
ORDER = (0, 7, 1, 2, 3, 4, 5, 6)
WINDOW = 3
A, B = 0, 1
PLANES = ((0, Q - 1), (Q - 1, 1))


def exchange(x, d, f, last, before, s, dv, fv, lev_out, lev_in, tot, from_even, pair, from_odd, pair_before,
             in_sem, lat_s, lat_r, lon_s, lon_r, lev_s, lev_r, even_s, even_r, odd_s, odd_r, back_s, back_r):
    la, lo, le = lax.axis_index("lat"), lax.axis_index("lon"), lax.axis_index("lev")
    lon_size, lev_size = lax.axis_size("lon"), lax.axis_size("lev")
    has_lon = (lo > 0, lo < lon_size - 1)
    has_lev = (le > 0, le < lev_size - 1)
    odd = lo % 2 == 1
    slots = lon_size // 2

    def load(n, q):
        j = q + la * (Q - 1 - 2 * q)
        if n == 0:
            return pltpu.make_async_copy(x.at[j], s.at[0, q + 1, pl.ds(1, N), pl.ds(PAD, K), :], in_sem.at[0, q])
        return pltpu.make_async_copy((d, f)[n - 1].at[j], (dv, fv)[n - 1].at[q], in_sem.at[n, q])

    load(0, Q - 1).start()
    for q in range(Q - 1):
        load(0, q).start()
    for q in range(Q):
        load(1, q).start()
        load(2, q).start()

    barrier = pltpu.get_barrier_semaphore()

    def greet(dev):
        pl.semaphore_signal(barrier, inc=1, device_id=dev, device_id_type=MESH)

    greet((1 - la, lo, le))
    count = jnp.int32(1)
    peers = [
        (has_lon[0], (la, lo - 1, le)),
        (has_lon[1], (la, lo + 1, le)),
        (has_lev[0], (la, lo, le - 1)),
        (has_lev[1], (la, lo, le + 1)),
    ]
    for far in range(1, slots):
        peers.append((odd & (lo >= 2 * far), (la, lo - 2 * far, le)))
        peers.append((odd & (lo + 2 * far < lon_size), (la, lo + 2 * far, le)))
    for there, dev in peers:
        count = count + there.astype(jnp.int32)

        @pl.when(there)
        def _():
            greet(dev)

    zero_row = jnp.zeros((K, M), jnp.float32)
    zero_cell = jnp.zeros((1, M), jnp.float32)

    @pl.loop(0, N)
    def _(i):
        for b in range(2):
            s[b, 0, i + 1, pl.ds(PAD, K), :] = zero_row

    for side, row in ((0, 0), (1, N + 1)):
        @pl.when(jnp.logical_not(has_lon[side]))
        def _():
            @pl.loop(0, Q)
            def _(q):
                for b in range(2):
                    s[b, q + 1, row, pl.ds(PAD, K), :] = zero_row

    for side, cell in ((0, PAD - 1), (1, TOP)):
        @pl.when(jnp.logical_not(has_lev[side]))
        def _():
            @pl.loop(0, Q)
            def _(q):
                @pl.loop(0, N)
                def _(i):
                    for b in range(2):
                        s[b, q + 1, i + 1, pl.ds(cell, 1), :] = zero_cell

    pl.semaphore_wait(barrier, count)

    def lat_copy(tick):
        t, c = tick // CHUNKS, ORDER[tick % CHUNKS]
        rows = pl.ds(1 + c * ROWS, ROWS)
        return pltpu.make_async_remote_copy(
            src_ref=s.at[t % 2, Q, rows, pl.ds(PAD, K), :],
            dst_ref=s.at[t % 2, Q + 1, rows, pl.ds(PAD, K), :],
            send_sem=lat_s.at[tick], recv_sem=lat_r.at[tick],
            device_id=(1 - la, lo, le), device_id_type=MESH)

    def lon_copy(t, group, side):
        q0, n = PLANES[group]
        src, dst = ((1, N + 1), (N, 0))[side]
        planes = pl.ds(q0 + 1, n)
        return pltpu.make_async_remote_copy(
            src_ref=s.at[t % 2, planes, src, pl.ds(PAD, K), :],
            dst_ref=s.at[t % 2, planes, dst, pl.ds(PAD, K), :],
            send_sem=lon_s.at[t, group, side], recv_sem=lon_r.at[t, group, side],
            device_id=(la, lo + (-1, 1)[side], le), device_id_type=MESH)

    def lev_copy(t, group, side):
        q0, n = PLANES[group]
        planes = pl.ds(q0, n)
        return pltpu.make_async_remote_copy(
            src_ref=lev_out.at[t % 2, side, planes],
            dst_ref=lev_in.at[t, side, planes],
            send_sem=lev_s.at[t, group, side], recv_sem=lev_r.at[t, group, side],
            device_id=(la, lo, le + (-1, 1)[side]), device_id_type=MESH)

    def send_lon(t, group, side):
        @pl.when(has_lon[side])
        def _():
            lon_copy(t, group, side).start()

    def send_lev(t, group):
        q0, n = PLANES[group]

        @pl.loop(q0, q0 + n)
        def _(q):
            @pl.loop(0, N)
            def _(i):
                lev_out[t % 2, 0, q, i] = s[t % 2, q + 1, i + 1, pl.ds(PAD, 1), :]
                lev_out[t % 2, 1, q, i] = s[t % 2, q + 1, i + 1, pl.ds(TOP - 1, 1), :]

        for side in range(2):
            @pl.when(has_lev[side])
            def _():
                lev_copy(t, group, side).start()

    def sent(t, group):
        for side in range(2):
            @pl.when(has_lon[side])
            def _():
                lon_copy(t, group, side).wait_send()

            @pl.when(has_lev[side])
            def _():
                lev_copy(t, group, side).wait_send()

    def arrived(t, group):
        q0, n = PLANES[group]
        for side in range(2):
            @pl.when(has_lon[1 - side])
            def _():
                lon_copy(t, group, side).wait_recv()

            @pl.when(has_lev[1 - side])
            def _():
                lev_copy(t, group, side).wait_recv()
                cell = (TOP, PAD - 1)[side]

                @pl.loop(q0, q0 + n)
                def _(q):
                    @pl.loop(0, N)
                    def _(i):
                        s[t % 2, q + 1, i + 1, pl.ds(cell, 1), :] = lev_in[t, side, q, i]

    def update(t, q, i):
        b = t % 2
        here = s.at[b, q + 1, i + 1]
        middle = here[pl.ds(PAD, K), :]
        spread = here[pl.ds(PAD - 1, K), :] + here[pl.ds(PAD + 1, K), :]
        spread += s[b, q + 1, i, pl.ds(PAD, K), :] + s[b, q + 1, i + 2, pl.ds(PAD, K), :]
        spread += s[b, q, i + 1, pl.ds(PAD, K), :] + s[b, q + 2, i + 1, pl.ds(PAD, K), :]
        new = middle + dv[q, i] * (spread - 6.0 * middle) + fv[q, i]
        if t == STEPS - 1:
            last[q, i] = new
        else:
            s[1 - b, q + 1, i + 1, pl.ds(PAD, K), :] = new
        return new

    def update_group_a(t):
        @pl.loop(0, Q - 1)
        def _(q):
            if t == STEPS - 1:
                def row(i, total):
                    return total + update(t, q, i)
                tot[q] = lax.fori_loop(0, N, row, zero_row)
            else:
                @pl.loop(0, N)
                def _(i):
                    update(t, q, i)

    def update_chunk(t, c):
        if t == STEPS - 1:
            def row(i, total):
                return total + update(t, Q - 1, i)
            total = lax.fori_loop(c * ROWS, (c + 1) * ROWS, row, zero_row)
            if c == ORDER[0]:
                tot[Q - 1] = total
            else:
                tot[Q - 1] = tot[Q - 1] + total
        else:
            @pl.loop(c * ROWS, (c + 1) * ROWS)
            def _(i):
                update(t, Q - 1, i)

    def even_copy(group):
        planes = pl.ds(*PLANES[group])
        return pltpu.make_async_remote_copy(
            src_ref=tot.at[planes], dst_ref=from_even.at[planes],
            send_sem=even_s.at[group], recv_sem=even_r.at[group],
            device_id=(la, lo + 1, le), device_id_type=MESH)

    def odd_copy(group, far, slot):
        planes = pl.ds(*PLANES[group])
        return pltpu.make_async_remote_copy(
            src_ref=pair.at[planes], dst_ref=from_odd.at[slot, planes],
            send_sem=odd_s.at[group, far], recv_sem=odd_r.at[group, slot],
            device_id=(la, lo + 2 * far, le), device_id_type=MESH)

    def back_copy(group):
        planes = pl.ds(*PLANES[group])
        return pltpu.make_async_remote_copy(
            src_ref=pair_before.at[planes], dst_ref=before.at[planes],
            send_sem=back_s.at[group], recv_sem=back_r.at[group],
            device_id=(la, lo - 1, le), device_id_type=MESH)

    def prefix_0(group):
        @pl.when(jnp.logical_not(odd))
        def _():
            even_copy(group).start()

    def prefix_1(group):
        q0, n = PLANES[group]

        @pl.when(odd)
        def _():
            even_copy(group).wait_recv()
            @pl.loop(q0, q0 + n)
            def _(q):
                pair[q] = tot[q] + from_even[q]

            for far in range(1, slots):
                @pl.when(lo + 2 * far < lon_size)
                def _():
                    odd_copy(group, far, far - 1).start()

    def prefix_2(group):
        q0, n = PLANES[group]

        @pl.when(odd)
        def _():
            @pl.loop(q0, q0 + n)
            def _(q):
                pair_before[q] = zero_row

            for far in range(1, slots):
                @pl.when(lo >= 2 * far)
                def _():
                    odd_copy(group, far, far - 1).wait_recv()

                    @pl.loop(q0, q0 + n)
                    def _(q):
                        pair_before[q] = pair_before[q] + from_odd[far - 1, q]

            back_copy(group).start()

            @pl.loop(q0, q0 + n)
            def _(q):
                before[q] = pair_before[q] + from_even[q]

    def prefix_3(group):
        @pl.when(odd)
        def _():
            back_copy(group).wait_send()
            for far in range(1, slots):
                @pl.when(lo + 2 * far < lon_size)
                def _():
                    odd_copy(group, far, far - 1).wait_send()

        @pl.when(jnp.logical_not(odd))
        def _():
            back_copy(group).wait_recv()
            even_copy(group).wait_send()

    load(0, Q - 1).wait()
    for tick in range(WINDOW):
        lat_copy(tick).start()
    for side in range(2):
        send_lon(0, B, side)
    send_lev(0, B)
    for q in range(Q - 1):
        load(0, q).wait()
    for side in range(2):
        send_lon(0, A, side)
    send_lev(0, A)
    for q in range(Q):
        load(1, q).wait()
        load(2, q).wait()

    ticks = STEPS * CHUNKS
    for t in range(STEPS):
        final = t == STEPS - 1
        arrived(t, A)
        if t > 0:
            sent(t - 1, A)
        update_group_a(t)
        if final:
            prefix_0(A)
        else:
            for side in range(2):
                send_lon(t + 1, A, side)
            send_lev(t + 1, A)
        arrived(t, B)
        if t > 0:
            sent(t - 1, B)
        for n in range(CHUNKS):
            tick, c = t * CHUNKS + n, ORDER[n]
            lat_copy(tick).wait_recv()
            if t > 0:
                lat_copy(tick - CHUNKS).wait_send()
            update_chunk(t, c)
            if not final:
                if c == 0:
                    send_lon(t + 1, B, 0)
                if c == CHUNKS - 1:
                    send_lon(t + 1, B, 1)
            if tick + WINDOW < ticks:
                lat_copy(tick + WINDOW).start()
            if final and n == 1:
                prefix_1(A)
            if final and n == CHUNKS - 2:
                prefix_2(A)
        if not final:
            send_lev(t + 1, B)
    prefix_0(B)
    prefix_1(B)
    prefix_2(B)
    for n in range(CHUNKS):
        lat_copy(ticks - CHUNKS + n).wait_send()
    for group in (A, B):
        sent(STEPS - 1, group)
        prefix_3(group)


def finish(last, before, totals, end, run, t_sem, c_sem):
    la = lax.axis_index("lat")
    scale = 1.0 / (N * lax.axis_size("lon"))

    def place(q):
        return q + la * (Q - 1 - 2 * q)

    def put_end(q):
        return pltpu.make_async_copy(last.at[q], end.at[place(q)], t_sem.at[q])

    def put_totals(q):
        return pltpu.make_async_copy(run.at[q], totals.at[place(q)], c_sem.at[q])

    for q in range(Q):
        put_end(q).start()
    for q in range(Q):
        def row(i, total):
            total = total + last[q, i]
            run[q, i] = total * scale
            return total
        lax.fori_loop(0, N, row, before[q])
        put_totals(q).start()
    for q in range(Q):
        put_end(q).wait()
        put_totals(q).wait()


def per_device(x, d, f):
    hbm = pl.BlockSpec(memory_space=pltpu.HBM)
    vmem = pl.BlockSpec(memory_space=pltpu.VMEM)
    slots = lax.axis_size("lon") // 2
    dma = pltpu.SemaphoreType.DMA
    block = (Q, N, K, M)
    part = (Q, K, M)
    f32 = jnp.float32
    last, before = pl.pallas_call(
        exchange,
        out_shape=(pltpu.VMEM(block, f32), pltpu.VMEM(part, f32)),
        in_specs=[hbm] * 3,
        out_specs=(vmem, vmem),
        scratch_shapes=[
            pltpu.VMEM((2, Q + 2, N + 2, K + 2 * PAD, M), f32),
            pltpu.VMEM(block, f32),
            pltpu.VMEM(block, f32),
            pltpu.VMEM((2, 2, Q, N, 1, M), f32),
            pltpu.VMEM((STEPS, 2, Q, N, 1, M), f32),
            pltpu.VMEM(part, f32),
            pltpu.VMEM(part, f32),
            pltpu.VMEM(part, f32),
            pltpu.VMEM((slots - 1,) + part, f32),
            pltpu.VMEM(part, f32),
            dma((3, Q)),
            dma((STEPS * CHUNKS,)), dma((STEPS * CHUNKS,)),
            dma((STEPS, 2, 2)), dma((STEPS, 2, 2)),
            dma((STEPS, 2, 2)), dma((STEPS, 2, 2)),
            dma((2,)), dma((2,)),
            dma((2, slots)), dma((2, slots)),
            dma((2,)), dma((2,)),
        ],
        compiler_params=pltpu.CompilerParams(
            collective_id=0, has_side_effects=True, vmem_limit_bytes=52 * 1024 * 1024),
        name="exchange",
    )(x, d, f)
    totals, end = pl.pallas_call(
        finish,
        out_shape=(jax.ShapeDtypeStruct(block, f32), jax.ShapeDtypeStruct(block, f32)),
        in_specs=[vmem, vmem],
        out_specs=(hbm, hbm),
        scratch_shapes=[pltpu.VMEM(block, f32), dma((Q,)), dma((Q,))],
        compiler_params=pltpu.CompilerParams(vmem_limit_bytes=16 * 1024 * 1024),
        name="finish",
    )(last, before)
    return totals, end


def solution(mesh):
    spec = P("lat", "lon", "lev", None)
    return jax.shard_map(
        per_device, mesh=mesh, in_specs=(spec,) * 3, out_specs=(spec, spec), check_vma=False)
```

```python
import jax
import jax.numpy as jnp
from jax import lax
from jax.experimental import pallas as pl
from jax.experimental.pallas import tpu as pltpu
from jax.sharding import PartitionSpec as P

STEPS = 4
MESH = pl.DeviceIdType.MESH
Q, N, K, M = 8, 32, 64, 128
PAD = 8
TOP = PAD + K
EDGE = Q - 1
CHUNKS = 8
ROWS = N // CHUNKS
ORDER = (0, 7, 1, 2, 3, 4, 5, 6)
WINDOW = 4
TICKS = STEPS * CHUNKS
RELAY = (2, 4, 6)
LATE = {2: (2, 0), 3: (3, 1), 4: (4,), 5: (5,), 6: (6,), 7: (7,)}
A, B = 0, 1
PLANES = ((0, Q - 1), (Q - 1, 1))


def exchange(x, d, f, last, before, s, dv, fv, hold, tot, from_even, pair, from_odd, pair_before,
             in_sem, lat_s, lat_r, lon_s, lon_r, lev_s, lev_r, hold_s, hold_r, turn_s,
             even_s, even_r, odd_s, odd_r, back_s, back_r):
    la, lo, le = lax.axis_index("lat"), lax.axis_index("lon"), lax.axis_index("lev")
    lon_size, lev_size = lax.axis_size("lon"), lax.axis_size("lev")
    half = lon_size // 2
    has_lon = (lo > 0, lo < lon_size - 1)
    has_lev = (le > 0, le < lev_size - 1)
    odd = lo % 2 == 1
    even = lo % 2 == 0
    near = (odd, even)
    wide = (even & (lo > 0), odd & (lo < lon_size - 1))
    slots = lon_size // 2
    cells = pl.ds(PAD, K)

    def load(n, q):
        j = q + la * (Q - 1 - 2 * q)
        if n == 0:
            return pltpu.make_async_copy(x.at[j], s.at[0, q + 1, pl.ds(1, N), cells, :], in_sem.at[0, q])
        return pltpu.make_async_copy((d, f)[n - 1].at[j], (dv, fv)[n - 1].at[q], in_sem.at[n, q])

    load(0, EDGE).start()
    for q in range(EDGE):
        load(0, q).start()

    barrier = pltpu.get_barrier_semaphore()

    def greet(dev):
        pl.semaphore_signal(barrier, inc=1, device_id=dev, device_id_type=MESH)

    greet((1 - la, lo, le))
    count = jnp.int32(1)
    peers = [
        (has_lon[0], (la, lo - 1, le)),
        (has_lon[1], (la, lo + 1, le)),
        (has_lev[0], (la, lo, le - 1)),
        (has_lev[1], (la, lo, le + 1)),
        (wide[0], (1 - la, lo - 1, le)),
        (wide[1], (1 - la, lo + 1, le)),
        (lo == 0, (la, half, le)),
        (lo == half, (la, 0, le)),
        (lo == 0, (la, half - 1, le)),
        (lo == half - 1, (la, 0, le)),
        (lo == lon_size - 1, (la, half, le)),
        (lo == half, (la, lon_size - 1, le)),
    ]
    for far in range(1, slots):
        peers.append((odd & (lo >= 2 * far), (la, lo - 2 * far, le)))
        peers.append((odd & (lo + 2 * far < lon_size), (la, lo + 2 * far, le)))
    for there, dev in peers:
        count = count + there.astype(jnp.int32)

        @pl.when(there)
        def _():
            greet(dev)

    zero_row = jnp.zeros((K, M), jnp.float32)
    zero_cell = jnp.zeros((1, M), jnp.float32)

    @pl.loop(0, N)
    def _(i):
        for b in range(2):
            s[b, 0, i + 1, cells, :] = zero_row

    for side, row in ((0, 0), (1, N + 1)):
        @pl.when(jnp.logical_not(has_lon[side]))
        def _():
            @pl.loop(0, Q)
            def _(q):
                for b in range(2):
                    s[b, q + 1, row, cells, :] = zero_row

    for side, cell in ((0, PAD - 1), (1, TOP)):
        @pl.when(jnp.logical_not(has_lev[side]))
        def _():
            @pl.loop(0, Q)
            def _(q):
                @pl.loop(0, N)
                def _(i):
                    for b in range(2):
                        s[b, q + 1, i + 1, pl.ds(cell, 1), :] = zero_cell

    pl.semaphore_wait(barrier, count)

    def lat_copy(tick):
        t, c = tick // CHUNKS, ORDER[tick % CHUNKS]
        rows = pl.ds(1 + c * ROWS, ROWS)
        return pltpu.make_async_remote_copy(
            src_ref=s.at[t % 2, Q, rows, cells, :],
            dst_ref=s.at[t % 2, Q + 1, rows, cells, :],
            send_sem=lat_s.at[tick], recv_sem=lat_r.at[tick],
            device_id=(1 - la, lo, le), device_id_type=MESH)

    FROM, TO = (1, N), (N + 1, 0)

    def lon_copy(t, q, side):
        return pltpu.make_async_remote_copy(
            src_ref=s.at[t % 2, q + 1, FROM[side], cells, :],
            dst_ref=s.at[t % 2, q + 1, TO[side], cells, :],
            send_sem=lon_s.at[t, q, side], recv_sem=lon_r.at[t, q, side],
            device_id=(la, lo + (-1, 1)[side], le), device_id_type=MESH)

    def hold_copy(t, q, side):
        r = RELAY.index(q)
        return pltpu.make_async_remote_copy(
            src_ref=s.at[t % 2, q + 1, FROM[side], cells, :],
            dst_ref=hold.at[t, r],
            send_sem=lon_s.at[t, q, side], recv_sem=hold_r.at[t, r],
            device_id=(la, lo + (-half, half)[side], le), device_id_type=MESH)

    def pass_copy(t, q, side):
        r = RELAY.index(q)
        return pltpu.make_async_remote_copy(
            src_ref=hold.at[t, r],
            dst_ref=s.at[t % 2, q + 1, TO[side], cells, :],
            send_sem=hold_s.at[t, r], recv_sem=lon_r.at[t, q, side],
            device_id=(la, lo + (half - 1, 1 - half)[side], le), device_id_type=MESH)

    def turn_copy(t, side):
        return pltpu.make_async_remote_copy(
            src_ref=s.at[t % 2, Q + 1, FROM[side], cells, :],
            dst_ref=s.at[t % 2, Q, TO[side], cells, :],
            send_sem=turn_s.at[t], recv_sem=lon_r.at[t, EDGE, side],
            device_id=(1 - la, lo + (-1, 1)[side], le), device_id_type=MESH)

    def lev_copy(t, q, side):
        return pltpu.make_async_remote_copy(
            src_ref=s.at[t % 2, q + 1, pl.ds(1, N), pl.ds((PAD, TOP - 1)[side], 1), :],
            dst_ref=s.at[t % 2, q + 1, pl.ds(1, N), pl.ds((TOP, PAD - 1)[side], 1), :],
            send_sem=lev_s.at[t, q, side], recv_sem=lev_r.at[t, q, side],
            device_id=(la, lo, le + (-1, 1)[side]), device_id_type=MESH)

    sender = (lo == half, lo == half - 1)
    keeper = (lo == 0, lo == lon_size - 1)

    def send_lev(t, q):
        for side in range(2):
            @pl.when(has_lev[side])
            def _():
                lev_copy(t, q, side).start()

    def send_lon(t, q):
        for side in range(2):
            if q in RELAY:
                @pl.when(has_lon[side] & jnp.logical_not(sender[side]))
                def _():
                    lon_copy(t, q, side).start()

                @pl.when(sender[side])
                def _():
                    hold_copy(t, q, side).start()
            else:
                @pl.when(has_lon[side])
                def _():
                    lon_copy(t, q, side).start()

    def send_near(t, side):
        @pl.when(near[side])
        def _():
            lon_copy(t, EDGE, side).start()

    def pass_on(t, q):
        for side in range(2):
            @pl.when(keeper[side])
            def _():
                hold_copy(t, q, side).wait_recv()
                pass_copy(t, q, side).start()

    def sent_lev(t, q):
        for side in range(2):
            @pl.when(has_lev[side])
            def _():
                lev_copy(t, q, side).wait_send()

    def sent_lon(t, q):
        for side in range(2):
            @pl.when(near[side] if q == EDGE else has_lon[side])
            def _():
                lon_copy(t, q, side).wait_send()

    def arrived_lev(t, q):
        for side in range(2):
            @pl.when(has_lev[1 - side])
            def _():
                lev_copy(t, q, side).wait_recv()

    def arrived_lon(t, q, side):
        @pl.when(has_lon[1 - side])
        def _():
            lon_copy(t, q, side).wait_recv()

    def update(t, q, i):
        b = t % 2
        here = s.at[b, q + 1, i + 1]
        middle = here[cells, :]
        spread = here[pl.ds(PAD - 1, K), :] + here[pl.ds(PAD + 1, K), :]
        spread += s[b, q + 1, i, cells, :] + s[b, q + 1, i + 2, cells, :]
        spread += s[b, q, i + 1, cells, :] + s[b, q + 2, i + 1, cells, :]
        new = middle + dv[q, i] * (spread - 6.0 * middle) + fv[q, i]
        if t == STEPS - 1:
            last[q, i] = new
        else:
            s[1 - b, q + 1, i + 1, cells, :] = new
        return new

    def update_plane(t, q):
        if t == STEPS - 1:
            def row(i, total):
                return total + update(t, q, i)
            tot[q] = lax.fori_loop(0, N, row, zero_row)
        else:
            @pl.loop(0, N)
            def _(i):
                update(t, q, i)

    def update_chunk(t, n):
        c = ORDER[n]
        if t == STEPS - 1:
            def row(i, total):
                return total + update(t, EDGE, i)
            total = lax.fori_loop(c * ROWS, (c + 1) * ROWS, row, zero_row)
            if n == LATE[2][0]:
                tot[EDGE] = total
            else:
                tot[EDGE] = tot[EDGE] + total
        else:
            @pl.loop(c * ROWS, (c + 1) * ROWS)
            def _(i):
                update(t, EDGE, i)

    def even_copy(group):
        planes = pl.ds(*PLANES[group])
        return pltpu.make_async_remote_copy(
            src_ref=tot.at[planes], dst_ref=from_even.at[planes],
            send_sem=even_s.at[group], recv_sem=even_r.at[group],
            device_id=(la, lo + 1, le), device_id_type=MESH)

    def odd_copy(group, far, slot):
        planes = pl.ds(*PLANES[group])
        return pltpu.make_async_remote_copy(
            src_ref=pair.at[planes], dst_ref=from_odd.at[slot, planes],
            send_sem=odd_s.at[group, far], recv_sem=odd_r.at[group, slot],
            device_id=(la, lo + 2 * far, le), device_id_type=MESH)

    def back_copy(group):
        planes = pl.ds(*PLANES[group])
        return pltpu.make_async_remote_copy(
            src_ref=pair_before.at[planes], dst_ref=before.at[planes],
            send_sem=back_s.at[group], recv_sem=back_r.at[group],
            device_id=(la, lo - 1, le), device_id_type=MESH)

    def prefix_0(group):
        @pl.when(jnp.logical_not(odd))
        def _():
            even_copy(group).start()

    def prefix_1(group):
        q0, n = PLANES[group]

        @pl.when(odd)
        def _():
            even_copy(group).wait_recv()
            @pl.loop(q0, q0 + n)
            def _(q):
                pair[q] = tot[q] + from_even[q]

            for far in range(1, slots):
                @pl.when(lo + 2 * far < lon_size)
                def _():
                    odd_copy(group, far, far - 1).start()

    def prefix_2(group):
        q0, n = PLANES[group]

        @pl.when(odd)
        def _():
            @pl.loop(q0, q0 + n)
            def _(q):
                pair_before[q] = zero_row

            for far in range(1, slots):
                @pl.when(lo >= 2 * far)
                def _():
                    odd_copy(group, far, far - 1).wait_recv()

                    @pl.loop(q0, q0 + n)
                    def _(q):
                        pair_before[q] = pair_before[q] + from_odd[far - 1, q]

            back_copy(group).start()

            @pl.loop(q0, q0 + n)
            def _(q):
                before[q] = pair_before[q] + from_even[q]

    def prefix_3(group):
        @pl.when(odd)
        def _():
            back_copy(group).wait_send()
            for far in range(1, slots):
                @pl.when(lo + 2 * far < lon_size)
                def _():
                    odd_copy(group, far, far - 1).wait_send()

        @pl.when(jnp.logical_not(odd))
        def _():
            back_copy(group).wait_recv()
            even_copy(group).wait_send()

    load(0, EDGE).wait()
    lat_copy(0).start()
    for q in (0, 1, EDGE, 2, 3, 4, 5, 6):
        load(1, q).start()
        load(2, q).start()
    send_lev(0, EDGE)
    for side in range(2):
        send_near(0, side)
    for q in range(EDGE):
        load(0, q).wait()
    lat_copy(1).start()
    for q in range(EDGE):
        send_lev(0, q)
        send_lon(0, q)
        if q in (2, 4):
            lat_copy(q // 2 + 1).start()
    for tick in range(4, WINDOW):
        lat_copy(tick).start()

    for t in range(STEPS):
        final = t == STEPS - 1
        for n in range(CHUNKS):
            tick = t * CHUNKS + n
            lat_copy(tick).wait_recv()
            if tick + WINDOW < TICKS:
                lat_copy(tick + WINDOW).start()
            if n < 2:
                @pl.when(wide[n])
                def _():
                    turn_copy(t, n).start()
            if t == 0 and n + 2 in RELAY:
                pass_on(0, n + 2)
            if not final and n - 1 in RELAY:
                pass_on(t + 1, n - 1)
            for m in LATE.get(n, ()):
                if t == 0 and n == 2 and m == n:
                    load(1, EDGE).wait()
                    load(2, EDGE).wait()
                if m == 2:
                    arrived_lev(t, EDGE)
                    if t > 0:
                        sent_lev(t - 1, EDGE)
                        sent_lon(t - 1, EDGE)
                if m < 2:
                    arrived_lon(t, EDGE, 1 - m)

                    @pl.when(wide[m])
                    def _():
                        turn_copy(t, m).wait_send()
                if t > 0:
                    lat_copy(tick - n + m - CHUNKS).wait_send()
                update_chunk(t, m)
                if not final and m < 2:
                    send_near(t + 1, m)
            planes = ((n,) if n < EDGE else ()) if not final else tuple(q for q in (2 * n, 2 * n + 1) if q < EDGE)
            for q in planes:
                if t == 0:
                    load(1, q).wait()
                    load(2, q).wait()
                arrived_lev(t, q)
                for side in range(2):
                    arrived_lon(t, q, side)
                if t > 0:
                    sent_lev(t - 1, q)
                    sent_lon(t - 1, q)
                update_plane(t, q)
                if not final:
                    send_lev(t + 1, q)
                    send_lon(t + 1, q)
            if final and n == 3:
                prefix_0(A)
            if final and n == 4:
                prefix_1(A)
        if not final:
            send_lev(t + 1, EDGE)
    prefix_0(B)
    prefix_1(B)
    prefix_2(A)
    prefix_2(B)
    for n in range(CHUNKS):
        lat_copy(TICKS - CHUNKS + n).wait_send()
    for q in range(Q):
        sent_lev(STEPS - 1, q)
        sent_lon(STEPS - 1, q)
    for t in range(STEPS):
        for q in RELAY:
            for side in range(2):
                @pl.when(keeper[side])
                def _():
                    pass_copy(t, q, side).wait_send()
    for group in (A, B):
        prefix_3(group)


def finish(last, before, totals, end, run, t_sem, c_sem):
    la = lax.axis_index("lat")
    scale = 1.0 / (N * lax.axis_size("lon"))

    def place(q):
        return q + la * (Q - 1 - 2 * q)

    def put_end(q):
        return pltpu.make_async_copy(last.at[q], end.at[place(q)], t_sem.at[q])

    def put_totals(q):
        return pltpu.make_async_copy(run.at[q], totals.at[place(q)], c_sem.at[q])

    for q in range(Q):
        put_end(q).start()
    for q in range(Q):
        def row(i, total):
            total = total + last[q, i]
            run[q, i] = total * scale
            return total
        lax.fori_loop(0, N, row, before[q])
        put_totals(q).start()
    for q in range(Q):
        put_end(q).wait()
        put_totals(q).wait()


def per_device(x, d, f):
    hbm = pl.BlockSpec(memory_space=pltpu.HBM)
    vmem = pl.BlockSpec(memory_space=pltpu.VMEM)
    slots = lax.axis_size("lon") // 2
    dma = pltpu.SemaphoreType.DMA
    block = (Q, N, K, M)
    part = (Q, K, M)
    f32 = jnp.float32
    last, before = pl.pallas_call(
        exchange,
        out_shape=(pltpu.VMEM(block, f32), pltpu.VMEM(part, f32)),
        in_specs=[hbm] * 3,
        out_specs=(vmem, vmem),
        scratch_shapes=[
            pltpu.VMEM((2, Q + 2, N + 2, K + 2 * PAD, M), f32),
            pltpu.VMEM(block, f32),
            pltpu.VMEM(block, f32),
            pltpu.VMEM((STEPS, len(RELAY), K, M), f32),
            pltpu.VMEM(part, f32),
            pltpu.VMEM(part, f32),
            pltpu.VMEM(part, f32),
            pltpu.VMEM((slots - 1,) + part, f32),
            pltpu.VMEM(part, f32),
            dma((3, Q)),
            dma((TICKS,)), dma((TICKS,)),
            dma((STEPS, Q, 2)), dma((STEPS, Q, 2)),
            dma((STEPS, Q, 2)), dma((STEPS, Q, 2)),
            dma((STEPS, len(RELAY))), dma((STEPS, len(RELAY))), dma((STEPS,)),
            dma((2,)), dma((2,)),
            dma((2, slots)), dma((2, slots)),
            dma((2,)), dma((2,)),
        ],
        compiler_params=pltpu.CompilerParams(
            collective_id=0, has_side_effects=True, vmem_limit_bytes=52 * 1024 * 1024),
        name="exchange",
    )(x, d, f)
    totals, end = pl.pallas_call(
        finish,
        out_shape=(jax.ShapeDtypeStruct(block, f32), jax.ShapeDtypeStruct(block, f32)),
        in_specs=[vmem, vmem],
        out_specs=(hbm, hbm),
        scratch_shapes=[pltpu.VMEM(block, f32), dma((Q,)), dma((Q,))],
        compiler_params=pltpu.CompilerParams(vmem_limit_bytes=16 * 1024 * 1024),
        name="finish",
    )(last, before)
    return totals, end


def solution(mesh):
    spec = P("lat", "lon", "lev", None)
    return jax.shard_map(
        per_device, mesh=mesh, in_specs=(spec,) * 3, out_specs=(spec, spec), check_vma=False)
```

```python
import jax
import jax.numpy as jnp
from jax import lax
from jax.experimental import pallas as pl
from jax.experimental.pallas import tpu as pltpu
from jax.sharding import PartitionSpec as P

STEPS = 4
MESH = pl.DeviceIdType.MESH
Q, N, K, M = 8, 32, 64, 128
PAD = 8
TOP = PAD + K
EDGE = Q - 1
CHUNKS = 8
ROWS = N // CHUNKS
ORDER = (0, 7, 1, 2, 3, 4, 5, 6)
WINDOW = 4
TICKS = STEPS * CHUNKS
GROUPS = ((0, 2), (2, 2), (4, 2), (6, 1), (7, 1))
LAST = len(GROUPS) - 1
RELAY = (1, 3)
LATE = {2: (2, 0), 3: (3, 1), 4: (4,), 5: (5,), 6: (6,), 7: (7,)}
PIECES = 4
A, B = 0, 1
PLANES = ((0, Q - 1), (Q - 1, 1))
GREET = ((1, range(7)), (2, (0, 1, 3, 4, 5)), (3, (0, 1, 3, 4)), (4, (0, 1, 2, 3)), (5, (1,)), (6, (1,)))


def exchange(x, d, f, last, before, s, dv, fv, hold, tot, mate, pair, joint, over_z, over_x, through, earlier,
             in_sem, pair_sem, lat_s, lat_r, lon_s, lon_r, lev_s, lev_r, hold_s, hold_r, turn_s,
             mate_s, mate_r, z_s, z_r, x_s, x_r, back_s, back_r, far_s, far_r):
    la, lo, le = lax.axis_index("lat"), lax.axis_index("lon"), lax.axis_index("lev")
    lon_size, lev_size = lax.axis_size("lon"), lax.axis_size("lev")
    half = lon_size // 2
    has_lon = (lo > 0, lo < lon_size - 1)
    has_lev = (le > 0, le < lev_size - 1)
    odd = lo % 2 == 1
    even = lo % 2 == 0
    near = (odd, even)
    wide = (even & (lo > 0), odd & (lo < lon_size - 1))
    slots = lon_size // 2
    cells = pl.ds(PAD, K)

    def place(q):
        return q + la * (Q - 1 - 2 * q)

    def load(q):
        return pltpu.make_async_copy(x.at[place(q)], s.at[0, q + 1, pl.ds(1, N), cells, :], in_sem.at[q])

    def load_pair(n, p):
        planes = pl.ds(2 * p + la * (Q - 2 - 4 * p), 2)
        return pltpu.make_async_copy((d, f)[n - 1].at[planes], (dv, fv)[n - 1].at[planes], pair_sem.at[n - 1, p])

    load(EDGE).start()

    barrier = pltpu.get_barrier_semaphore()

    def greet(dev):
        pl.semaphore_signal(barrier, inc=1, device_id=dev, device_id_type=MESH)

    def among(members):
        found = lo < 0
        for m in members:
            found = found | (lo == m)
        return found

    greet((1 - la, lo, le))
    count = jnp.int32(1)
    peers = [
        (has_lev[0], (la, lo, le - 1)),
        (has_lev[1], (la, lo, le + 1)),
        (wide[0], (1 - la, lo - 1, le)),
        (wide[1], (1 - la, lo + 1, le)),
    ]
    for offset, lower in GREET:
        peers.append((among(lower), (la, lo + offset, le)))
        peers.append((among([m + offset for m in lower]), (la, lo - offset, le)))
    for there, dev in peers:
        count = count + there.astype(jnp.int32)

        @pl.when(there)
        def _():
            greet(dev)

    for q in range(EDGE):
        load(q).start()
    pl.semaphore_wait(barrier, count)

    zero_row = jnp.zeros((K, M), jnp.float32)
    zero_cell = jnp.zeros((1, M), jnp.float32)

    def lat_copy(tick):
        t, c = tick // CHUNKS, ORDER[tick % CHUNKS]
        rows = pl.ds(1 + c * ROWS, ROWS)
        return pltpu.make_async_remote_copy(
            src_ref=s.at[t % 2, Q, rows, cells, :],
            dst_ref=s.at[t % 2, Q + 1, rows, cells, :],
            send_sem=lat_s.at[tick % CHUNKS], recv_sem=lat_r.at[tick % CHUNKS],
            device_id=(1 - la, lo, le), device_id_type=MESH)

    FROM, TO = (1, N), (N + 1, 0)

    def face(t, g, i):
        q, n = GROUPS[g]
        return s.at[t % 2, pl.ds(q + 1, n), i, cells, :]

    def lon_copy(t, g, side):
        return pltpu.make_async_remote_copy(
            src_ref=face(t, g, FROM[side]), dst_ref=face(t, g, TO[side]),
            send_sem=lon_s.at[t % 2, g, side], recv_sem=lon_r.at[t % 2, g, side],
            device_id=(la, lo + (-1, 1)[side], le), device_id_type=MESH)

    def held(t, g):
        r = RELAY.index(g)
        return hold.at[t, pl.ds(2 * r, GROUPS[g][1])], t % 2, r

    def hold_copy(t, g, side):
        buffer, b, r = held(t, g)
        return pltpu.make_async_remote_copy(
            src_ref=face(t, g, FROM[side]), dst_ref=buffer,
            send_sem=lon_s.at[b, g, side], recv_sem=hold_r.at[b, r],
            device_id=(la, lo + (-half, half)[side], le), device_id_type=MESH)

    def pass_copy(t, g, side):
        buffer, b, r = held(t, g)
        return pltpu.make_async_remote_copy(
            src_ref=buffer, dst_ref=face(t, g, TO[side]),
            send_sem=hold_s.at[b, r], recv_sem=lon_r.at[b, g, side],
            device_id=(la, lo + (half - 1, 1 - half)[side], le), device_id_type=MESH)

    def turn_copy(t, side):
        return pltpu.make_async_remote_copy(
            src_ref=s.at[t % 2, Q + 1, FROM[side], cells, :],
            dst_ref=s.at[t % 2, Q, TO[side], cells, :],
            send_sem=turn_s, recv_sem=lon_r.at[t % 2, LAST, side],
            device_id=(1 - la, lo + (-1, 1)[side], le), device_id_type=MESH)

    def lev_copy(t, g, side):
        q, n = GROUPS[g]
        planes = pl.ds(q + 1, n)
        return pltpu.make_async_remote_copy(
            src_ref=s.at[t % 2, planes, pl.ds(1, N), pl.ds((PAD, TOP - 1)[side], 1), :],
            dst_ref=s.at[t % 2, planes, pl.ds(1, N), pl.ds((TOP, PAD - 1)[side], 1), :],
            send_sem=lev_s.at[t % 2, g, side], recv_sem=lev_r.at[t % 2, g, side],
            device_id=(la, lo, le + (-1, 1)[side]), device_id_type=MESH)

    sender = (lo == half, lo == half - 1)
    keeper = (lo == 0, lo == lon_size - 1)

    def send_lev(t, q):
        for side in range(2):
            @pl.when(has_lev[side])
            def _():
                lev_copy(t, q, side).start()

    def send_lon(t, q):
        for side in range(2):
            if q in RELAY:
                @pl.when(has_lon[side] & jnp.logical_not(sender[side]))
                def _():
                    lon_copy(t, q, side).start()

                @pl.when(sender[side])
                def _():
                    hold_copy(t, q, side).start()
            else:
                @pl.when(has_lon[side])
                def _():
                    lon_copy(t, q, side).start()

    def send_near(t, side):
        @pl.when(near[side])
        def _():
            lon_copy(t, LAST, side).start()

    def pass_on(t, q):
        for side in range(2):
            @pl.when(keeper[side])
            def _():
                if t > 1:
                    pass_copy(t - 2, q, side).wait_send()
                hold_copy(t, q, side).wait_recv()
                pass_copy(t, q, side).start()

    def sent_lev(t, q):
        for side in range(2):
            @pl.when(has_lev[side])
            def _():
                lev_copy(t, q, side).wait_send()

    def sent_lon(t, q):
        for side in range(2):
            @pl.when(near[side] if q == LAST else has_lon[side])
            def _():
                lon_copy(t, q, side).wait_send()

    def arrived_lev(t, q):
        for side in range(2):
            @pl.when(has_lev[1 - side])
            def _():
                lev_copy(t, q, side).wait_recv()

    def arrived_lon(t, q, side):
        @pl.when(has_lon[1 - side])
        def _():
            lon_copy(t, q, side).wait_recv()

    def update(t, q, i):
        b = t % 2
        here = s.at[b, q + 1, i + 1]
        middle = here[cells, :]
        spread = here[pl.ds(PAD - 1, K), :] + here[pl.ds(PAD + 1, K), :]
        spread += s[b, q + 1, i, cells, :] + s[b, q + 1, i + 2, cells, :]
        spread += s[b, q, i + 1, cells, :] + s[b, q + 2, i + 1, cells, :]
        j = place(q)
        new = middle + dv[j, i] * (spread - 6.0 * middle) + fv[j, i]
        if t == STEPS - 1:
            last[j, i] = new
        else:
            s[1 - b, q + 1, i + 1, cells, :] = new
        return new

    def update_plane(t, q):
        if t == STEPS - 1:
            def add(i, total):
                return total + update(t, q, i)
            tot[q] = lax.fori_loop(0, N, add, zero_row)
        else:
            @pl.loop(0, N)
            def _(i):
                update(t, q, i)

    def update_chunk(t, n):
        c = ORDER[n]
        if t == STEPS - 1:
            def add(i, total):
                return total + update(t, EDGE, i)
            total = lax.fori_loop(c * ROWS, (c + 1) * ROWS, add, zero_row)
            if n == LATE[2][0]:
                tot[EDGE] = total
            else:
                tot[EDGE] = tot[EDGE] + total
        else:
            @pl.loop(c * ROWS, (c + 1) * ROWS)
            def _(i):
                update(t, EDGE, i)

    def mate_copy(group):
        planes = pl.ds(*PLANES[group])
        return pltpu.make_async_remote_copy(
            src_ref=tot.at[planes], dst_ref=mate.at[planes],
            send_sem=mate_s.at[group], recv_sem=mate_r.at[group],
            device_id=(la, lo + (-1, 1)[group], le), device_id_type=MESH)

    rest = pl.ds(*PLANES[A])

    def z_copy():
        return pltpu.make_async_remote_copy(
            src_ref=pair, dst_ref=over_z, send_sem=z_s, recv_sem=z_r,
            device_id=(la, lo + half, le), device_id_type=MESH)

    def x_copy(source, offset):
        return pltpu.make_async_remote_copy(
            src_ref=source, dst_ref=over_x, send_sem=x_s, recv_sem=x_r,
            device_id=(la, lo + offset, le), device_id_type=MESH)

    def back_copy():
        return pltpu.make_async_remote_copy(
            src_ref=through, dst_ref=before.at[rest], send_sem=back_s, recv_sem=back_r,
            device_id=(la, lo + 1, le), device_id_type=MESH)

    def far_copy(far, to_odd):
        return pltpu.make_async_remote_copy(
            src_ref=joint, dst_ref=earlier.at[far - 1],
            send_sem=far_s.at[far - 1, to_odd], recv_sem=far_r.at[far - 1],
            device_id=(la, lo + 2 * far - 1 + to_odd, le), device_id_type=MESH)

    low_even = even & (lo < half)

    def rest_0():
        @pl.when(odd)
        def _():
            mate_copy(A).start()

    def rest_1():
        @pl.when(even)
        def _():
            mate_copy(A).wait_recv()

            @pl.loop(0, EDGE)
            def _(q):
                pair[q] = tot[q] + mate[q]

        @pl.when(lo == 0)
        def _():
            x_copy(pair, 2).start()

        @pl.when(low_even)
        def _():
            z_copy().start()

    def rest_2():
        @pl.when(lo == half)
        def _():
            z_copy().wait_recv()

            @pl.loop(0, EDGE)
            def _(q):
                pair[q] = pair[q] + over_z[q]

            x_copy(pair, 2).start()

        @pl.when(lo == half + 2)
        def _():
            z_copy().wait_recv()
            x_copy(over_z, -2).start()

    def rest_3():
        @pl.when(even & (lo > 0))
        def _():
            x_copy(pair, 2).wait_recv()

        @pl.when(lo == 0)
        def _():
            @pl.loop(0, EDGE)
            def _(q):
                before[q] = zero_row

        @pl.when(even & (lo > 0))
        def _():
            @pl.loop(0, EDGE)
            def _(q):
                before[q] = over_x[q]

        @pl.when(even & (lo >= half))
        def _():
            @pl.loop(0, EDGE)
            def _(q):
                before[q] = before[q] + over_z[q]

        @pl.when(even)
        def _():
            @pl.loop(0, EDGE)
            def _(q):
                through[q] = before[q] + tot[q]

            back_copy().start()

    def edge_0():
        @pl.when(even)
        def _():
            mate_copy(B).start()

    FARS = (3, 1, 2)

    def edge_1():
        @pl.when(odd)
        def _():
            mate_copy(B).wait_recv()
            joint[...] = tot[EDGE] + mate[EDGE]
            for far in FARS:
                @pl.when(lo + 2 * far < lon_size)
                def _():
                    far_copy(far, 1).start()
                    far_copy(far, 0).start()

    def edge_2():
        before[EDGE] = zero_row
        for far in range(1, slots):
            @pl.when(lo >= 2 * far)
            def _():
                far_copy(far, 1).wait_recv()
                before[EDGE] = before[EDGE] + earlier[far - 1]

        @pl.when(odd)
        def _():
            before[EDGE] = before[EDGE] + mate[EDGE]

    def prefix_end():
        @pl.when(odd)
        def _():
            back_copy().wait_recv()
            mate_copy(A).wait_send()
            for far in FARS:
                @pl.when(lo + 2 * far < lon_size)
                def _():
                    far_copy(far, 1).wait_send()
                    far_copy(far, 0).wait_send()

        @pl.when(even)
        def _():
            back_copy().wait_send()
            mate_copy(B).wait_send()

        @pl.when(low_even)
        def _():
            z_copy().wait_send()

        @pl.when(among((0, half, half + 2)))
        def _():
            x_copy(pair, 2).wait_send()

    def send_lat(tick):
        if tick >= CHUNKS:
            lat_copy(tick - CHUNKS).wait_send()
        lat_copy(tick).start()

    load(EDGE).wait()
    send_lat(0)
    send_lat(1)
    for p in (0, 3, 1, 2):
        load_pair(1, p).start()
        load_pair(2, p).start()
    send_lev(0, LAST)
    for side in range(2):
        send_near(0, side)

    @pl.loop(0, N)
    def _(i):
        for b in range(2):
            s[b, 0, i + 1, cells, :] = zero_row

    for side, row in ((0, 0), (1, N + 1)):
        @pl.when(jnp.logical_not(has_lon[side]))
        def _():
            @pl.loop(0, Q)
            def _(q):
                for b in range(2):
                    s[b, q + 1, row, cells, :] = zero_row

    for side, cell in ((0, PAD - 1), (1, TOP)):
        @pl.when(jnp.logical_not(has_lev[side]))
        def _():
            @pl.loop(0, Q)
            def _(q):
                @pl.loop(0, N)
                def _(i):
                    for b in range(2):
                        s[b, q + 1, i + 1, pl.ds(cell, 1), :] = zero_cell

    for g in range(LAST):
        q0, planes = GROUPS[g]
        for q in range(q0, q0 + planes):
            load(q).wait()
        send_lev(0, g)
        send_lon(0, g)
        if g < 2:
            send_lat(g + 2)

    for t in range(STEPS):
        final = t == STEPS - 1
        for n in range(CHUNKS):
            tick = t * CHUNKS + n
            lat_copy(tick).wait_recv()
            if tick + WINDOW < TICKS:
                send_lat(tick + WINDOW)
            if n < 2:
                @pl.when(wide[n])
                def _():
                    turn_copy(t, n).start()
            if t == 0 and n in (1, 4):
                pass_on(0, {1: 1, 4: 3}[n])
            if not final and n in (4, 7):
                pass_on(t + 1, {4: 1, 7: 3}[n])
            for m in LATE.get(n, ()):
                if m == 2:
                    if t == 0:
                        load_pair(1, 3).wait()
                        load_pair(2, 3).wait()
                    arrived_lev(t, LAST)
                    if t > 0:
                        sent_lev(t - 1, LAST)
                        sent_lon(t - 1, LAST)
                if m < 2:
                    arrived_lon(t, LAST, 1 - m)

                    @pl.when(wide[m])
                    def _():
                        turn_copy(t, m).wait_send()
                update_chunk(t, m)
                if not final and m < 2:
                    send_near(t + 1, m)
            planes = ((n,) if n < EDGE else ()) if not final else tuple(q for q in (2 * n, 2 * n + 1) if q < EDGE)
            for q in planes:
                g = q // 2
                first, count = GROUPS[g]
                if q == first:
                    if t == 0 and g < 3:
                        load_pair(1, g).wait()
                        load_pair(2, g).wait()
                    arrived_lev(t, g)
                    for side in range(2):
                        arrived_lon(t, g, side)
                    if t > 0:
                        sent_lev(t - 1, g)
                        sent_lon(t - 1, g)
                update_plane(t, q)
                if not final and q == first + count - 1:
                    send_lev(t + 1, g)
                    send_lon(t + 1, g)
            if final and n in (3, 4, 6):
                (rest_0, rest_1, rest_2)[(3, 4, 6).index(n)]()
        if not final:
            send_lev(t + 1, LAST)
    edge_0()
    edge_1()
    rest_3()
    edge_2()
    for n in range(CHUNKS):
        lat_copy(TICKS - CHUNKS + n).wait_send()
    for g in range(len(GROUPS)):
        sent_lev(STEPS - 1, g)
        sent_lon(STEPS - 1, g)
    for t in (STEPS - 2, STEPS - 1):
        for g in RELAY:
            for side in range(2):
                @pl.when(keeper[side])
                def _():
                    pass_copy(t, g, side).wait_send()
    prefix_end()


def finish(last, before, totals, end, run, t_sem, c_sem):
    la = lax.axis_index("lat")
    scale = 1.0 / (N * lax.axis_size("lon"))

    def place(q):
        return q + la * (Q - 1 - 2 * q)

    def put_end(p):
        planes = pl.ds(p * (Q // PIECES), Q // PIECES)
        return pltpu.make_async_copy(last.at[planes], end.at[planes], t_sem.at[p])

    def put_totals(q):
        return pltpu.make_async_copy(run.at[q], totals.at[place(q)], c_sem.at[q])

    for p in range(PIECES):
        put_end(p).start()
    for q in range(Q):
        def row(i, total):
            total = total + last[place(q), i]
            run[q, i] = total * scale
            return total
        lax.fori_loop(0, N, row, before[q])
        put_totals(q).start()
    for p in range(PIECES):
        put_end(p).wait()
    for q in range(Q):
        put_totals(q).wait()


def per_device(x, d, f):
    hbm = pl.BlockSpec(memory_space=pltpu.HBM)
    vmem = pl.BlockSpec(memory_space=pltpu.VMEM)
    slots = lax.axis_size("lon") // 2
    dma = pltpu.SemaphoreType.DMA
    block = (Q, N, K, M)
    part = (Q, K, M)
    f32 = jnp.float32
    last, before = pl.pallas_call(
        exchange,
        out_shape=(pltpu.VMEM(block, f32), pltpu.VMEM(part, f32)),
        in_specs=[hbm] * 3,
        out_specs=(vmem, vmem),
        scratch_shapes=[
            pltpu.VMEM((2, Q + 2, N + 2, K + 2 * PAD, M), f32),
            pltpu.VMEM(block, f32),
            pltpu.VMEM(block, f32),
            pltpu.VMEM((STEPS, 2 * len(RELAY), K, M), f32),
            pltpu.VMEM(part, f32),
            pltpu.VMEM(part, f32),
            pltpu.VMEM((EDGE, K, M), f32),
            pltpu.VMEM((K, M), f32),
            pltpu.VMEM((EDGE, K, M), f32),
            pltpu.VMEM((EDGE, K, M), f32),
            pltpu.VMEM((EDGE, K, M), f32),
            pltpu.VMEM((slots - 1, K, M), f32),
            dma((Q,)), dma((2, Q // 2)),
            dma((CHUNKS,)), dma((CHUNKS,)),
            dma((2, len(GROUPS), 2)), dma((2, len(GROUPS), 2)),
            dma((2, len(GROUPS), 2)), dma((2, len(GROUPS), 2)),
            dma((2, len(RELAY))), dma((2, len(RELAY))), dma,
            dma((2,)), dma((2,)), dma, dma, dma, dma, dma, dma,
            dma((slots - 1, 2)), dma((slots - 1,)),
        ],
        compiler_params=pltpu.CompilerParams(
            collective_id=0, has_side_effects=True, vmem_limit_bytes=52 * 1024 * 1024),
        name="exchange",
    )(x, d, f)
    totals, end = pl.pallas_call(
        finish,
        out_shape=(jax.ShapeDtypeStruct(block, f32), jax.ShapeDtypeStruct(block, f32)),
        in_specs=[vmem, vmem],
        out_specs=(hbm, hbm),
        scratch_shapes=[pltpu.VMEM(block, f32), dma((PIECES,)), dma((Q,))],
        compiler_params=pltpu.CompilerParams(vmem_limit_bytes=16 * 1024 * 1024),
        name="finish",
    )(last, before)
    return totals, end


def solution(mesh):
    spec = P("lat", "lon", "lev", None)
    return jax.shard_map(
        per_device, mesh=mesh, in_specs=(spec,) * 3, out_specs=(spec, spec), check_vma=False)
```

```python
import jax
import jax.numpy as jnp
from jax import lax
from jax.experimental import pallas as pl
from jax.experimental.pallas import tpu as pltpu
from jax.sharding import PartitionSpec as P

STEPS = 4
MESH = pl.DeviceIdType.MESH
Q, N, K, M = 8, 32, 64, 128
PAD = 8
TOP = PAD + K
EDGE = Q - 1
CHUNKS = 8
ROWS = N // CHUNKS
ORDER = (0, 7, 1, 2, 3, 4, 5, 6)
WINDOW = 4
TICKS = STEPS * CHUNKS
GROUPS = ((0, 4), (4, 3), (7, 1))
LAST = len(GROUPS) - 1
RELAY = (1,)
LATE = {2: (2, 0), 3: (3, 1), 4: (4,), 5: (5,), 6: (6,), 7: (7,)}
PIECES = 4
A, B = 0, 1
PASS = 5
PLANES = ((0, Q - 1), (Q - 1, 1))
GREET = ((1, range(7)), (2, (0, 1, 3, 4, 5)), (3, (0, 1, 3, 4)), (4, (0, 1, 2, 3)), (5, (1,)), (6, (1,)))


def exchange(x, d, f, last, before, s, dv, fv, hold, tot, mate, pair, joint, over_z, over_x, through, earlier,
             in_sem, pair_sem, lat_s, lat_r, lon_s, lon_r, lev_s, lev_r, hold_s, hold_r, turn_s,
             mate_s, mate_r, z_s, z_r, x_s, x_r, back_s, back_r, far_s, far_r):
    la, lo, le = lax.axis_index("lat"), lax.axis_index("lon"), lax.axis_index("lev")
    lon_size, lev_size = lax.axis_size("lon"), lax.axis_size("lev")
    half = lon_size // 2
    has_lon = (lo > 0, lo < lon_size - 1)
    has_lev = (le > 0, le < lev_size - 1)
    odd = lo % 2 == 1
    even = lo % 2 == 0
    near = (odd, even)
    wide = (even & (lo > 0), odd & (lo < lon_size - 1))
    slots = lon_size // 2
    cells = pl.ds(PAD, K)

    def place(q):
        return q + la * (Q - 1 - 2 * q)

    def load(q):
        return pltpu.make_async_copy(x.at[place(q)], s.at[0, q + 1, pl.ds(1, N), cells, :], in_sem.at[q])

    def load_pair(n, p):
        planes = pl.ds(2 * p + la * (Q - 2 - 4 * p), 2)
        return pltpu.make_async_copy((d, f)[n - 1].at[planes], (dv, fv)[n - 1].at[planes], pair_sem.at[n - 1, p])

    load(EDGE).start()

    barrier = pltpu.get_barrier_semaphore()

    def greet(dev):
        pl.semaphore_signal(barrier, inc=1, device_id=dev, device_id_type=MESH)

    def among(members):
        found = lo < 0
        for m in members:
            found = found | (lo == m)
        return found

    greet((1 - la, lo, le))
    count = jnp.int32(1)
    peers = [
        (has_lev[0], (la, lo, le - 1)),
        (has_lev[1], (la, lo, le + 1)),
        (wide[0], (1 - la, lo - 1, le)),
        (wide[1], (1 - la, lo + 1, le)),
    ]
    for offset, lower in GREET:
        peers.append((among(lower), (la, lo + offset, le)))
        peers.append((among([m + offset for m in lower]), (la, lo - offset, le)))
    for there, dev in peers:
        count = count + there.astype(jnp.int32)

        @pl.when(there)
        def _():
            greet(dev)

    for q in range(EDGE):
        load(q).start()
    pl.semaphore_wait(barrier, count)

    zero_row = jnp.zeros((K, M), jnp.float32)
    zero_cell = jnp.zeros((1, M), jnp.float32)

    def lat_copy(tick):
        t, c = tick // CHUNKS, ORDER[tick % CHUNKS]
        rows = pl.ds(1 + c * ROWS, ROWS)
        return pltpu.make_async_remote_copy(
            src_ref=s.at[t % 2, Q, rows, cells, :],
            dst_ref=s.at[t % 2, Q + 1, rows, cells, :],
            send_sem=lat_s.at[tick % CHUNKS], recv_sem=lat_r.at[tick % CHUNKS],
            device_id=(1 - la, lo, le), device_id_type=MESH)

    FROM, TO = (1, N), (N + 1, 0)

    def face(t, g, i):
        q, n = GROUPS[g]
        return s.at[t % 2, pl.ds(q + 1, n), i, cells, :]

    def lon_copy(t, g, side):
        return pltpu.make_async_remote_copy(
            src_ref=face(t, g, FROM[side]), dst_ref=face(t, g, TO[side]),
            send_sem=lon_s.at[t % 2, g, side], recv_sem=lon_r.at[t % 2, g, side],
            device_id=(la, lo + (-1, 1)[side], le), device_id_type=MESH)

    def held(t, g):
        r = RELAY.index(g)
        return hold.at[t, r, pl.ds(0, GROUPS[g][1])], t % 2, r

    def hold_copy(t, g, side):
        buffer, b, r = held(t, g)
        return pltpu.make_async_remote_copy(
            src_ref=face(t, g, FROM[side]), dst_ref=buffer,
            send_sem=lon_s.at[b, g, side], recv_sem=hold_r.at[b, r],
            device_id=(la, lo + (-half, half)[side], le), device_id_type=MESH)

    def pass_copy(t, g, side):
        buffer, b, r = held(t, g)
        return pltpu.make_async_remote_copy(
            src_ref=buffer, dst_ref=face(t, g, TO[side]),
            send_sem=hold_s.at[b, r], recv_sem=lon_r.at[b, g, side],
            device_id=(la, lo + (half - 1, 1 - half)[side], le), device_id_type=MESH)

    def turn_copy(t, side):
        return pltpu.make_async_remote_copy(
            src_ref=s.at[t % 2, Q + 1, FROM[side], cells, :],
            dst_ref=s.at[t % 2, Q, TO[side], cells, :],
            send_sem=turn_s, recv_sem=lon_r.at[t % 2, LAST, side],
            device_id=(1 - la, lo + (-1, 1)[side], le), device_id_type=MESH)

    def lev_copy(t, g, side):
        q, n = GROUPS[g]
        planes = pl.ds(q + 1, n)
        return pltpu.make_async_remote_copy(
            src_ref=s.at[t % 2, planes, pl.ds(1, N), pl.ds((PAD, TOP - 1)[side], 1), :],
            dst_ref=s.at[t % 2, planes, pl.ds(1, N), pl.ds((TOP, PAD - 1)[side], 1), :],
            send_sem=lev_s.at[t % 2, g, side], recv_sem=lev_r.at[t % 2, g, side],
            device_id=(la, lo, le + (-1, 1)[side]), device_id_type=MESH)

    sender = (lo == half, lo == half - 1)
    keeper = (lo == 0, lo == lon_size - 1)

    def send_lev(t, q):
        for side in range(2):
            @pl.when(has_lev[side])
            def _():
                lev_copy(t, q, side).start()

    def send_lon(t, q):
        for side in range(2):
            if q in RELAY:
                @pl.when(has_lon[side] & jnp.logical_not(sender[side]))
                def _():
                    lon_copy(t, q, side).start()

                @pl.when(sender[side])
                def _():
                    hold_copy(t, q, side).start()
            else:
                @pl.when(has_lon[side])
                def _():
                    lon_copy(t, q, side).start()

    def send_near(t, side):
        @pl.when(near[side])
        def _():
            lon_copy(t, LAST, side).start()

    def pass_on(t, q):
        for side in range(2):
            @pl.when(keeper[side])
            def _():
                if t > 1:
                    pass_copy(t - 2, q, side).wait_send()
                hold_copy(t, q, side).wait_recv()
                pass_copy(t, q, side).start()

    def sent_lev(t, q):
        for side in range(2):
            @pl.when(has_lev[side])
            def _():
                lev_copy(t, q, side).wait_send()

    def sent_lon(t, q):
        for side in range(2):
            @pl.when(near[side] if q == LAST else has_lon[side])
            def _():
                lon_copy(t, q, side).wait_send()

    def arrived_lev(t, q):
        for side in range(2):
            @pl.when(has_lev[1 - side])
            def _():
                lev_copy(t, q, side).wait_recv()

    def arrived_lon(t, q, side):
        @pl.when(has_lon[1 - side])
        def _():
            lon_copy(t, q, side).wait_recv()

    def update(t, q, i):
        b = t % 2
        here = s.at[b, q + 1, i + 1]
        middle = here[cells, :]
        spread = here[pl.ds(PAD - 1, K), :] + here[pl.ds(PAD + 1, K), :]
        spread += s[b, q + 1, i, cells, :] + s[b, q + 1, i + 2, cells, :]
        spread += s[b, q, i + 1, cells, :] + s[b, q + 2, i + 1, cells, :]
        j = place(q)
        new = middle + dv[j, i] * (spread - 6.0 * middle) + fv[j, i]
        if t == STEPS - 1:
            last[j, i] = new
        else:
            s[1 - b, q + 1, i + 1, cells, :] = new
        return new

    def update_plane(t, q):
        if t == STEPS - 1:
            def add(i, total):
                return total + update(t, q, i)
            tot[q] = lax.fori_loop(0, N, add, zero_row)
        else:
            @pl.loop(0, N)
            def _(i):
                update(t, q, i)

    def update_chunk(t, n):
        c = ORDER[n]
        if t == STEPS - 1:
            def add(i, total):
                return total + update(t, EDGE, i)
            total = lax.fori_loop(c * ROWS, (c + 1) * ROWS, add, zero_row)
            if n == LATE[2][0]:
                tot[EDGE] = total
            else:
                tot[EDGE] = tot[EDGE] + total
        else:
            @pl.loop(c * ROWS, (c + 1) * ROWS)
            def _(i):
                update(t, EDGE, i)

    def mate_copy(group):
        planes = pl.ds(*PLANES[group])
        return pltpu.make_async_remote_copy(
            src_ref=tot.at[planes], dst_ref=mate.at[planes],
            send_sem=mate_s.at[group], recv_sem=mate_r.at[group],
            device_id=(la, lo + (-1, 1)[group], le), device_id_type=MESH)

    rest = pl.ds(*PLANES[A])

    def z_copy():
        return pltpu.make_async_remote_copy(
            src_ref=pair, dst_ref=over_z, send_sem=z_s, recv_sem=z_r,
            device_id=(la, lo + half, le), device_id_type=MESH)

    def x_copy(source, offset):
        return pltpu.make_async_remote_copy(
            src_ref=source, dst_ref=over_x, send_sem=x_s, recv_sem=x_r,
            device_id=(la, lo + offset, le), device_id_type=MESH)

    def back_copy():
        return pltpu.make_async_remote_copy(
            src_ref=through, dst_ref=before.at[rest], send_sem=back_s, recv_sem=back_r,
            device_id=(la, lo + 1, le), device_id_type=MESH)

    def far_copy(far, to_odd):
        return pltpu.make_async_remote_copy(
            src_ref=joint, dst_ref=earlier.at[far - 1],
            send_sem=far_s.at[far - 1, to_odd], recv_sem=far_r.at[far - 1],
            device_id=(la, lo + 2 * far - 1 + to_odd, le), device_id_type=MESH)

    low_even = even & (lo < half)

    def rest_0():
        @pl.when(odd)
        def _():
            mate_copy(A).start()

    def rest_1():
        @pl.when(even)
        def _():
            mate_copy(A).wait_recv()

            @pl.loop(0, EDGE)
            def _(q):
                pair[q] = tot[q] + mate[q]

        @pl.when(lo == 0)
        def _():
            x_copy(pair, 2).start()

        @pl.when(low_even)
        def _():
            z_copy().start()

    def rest_2():
        @pl.when(lo == half)
        def _():
            z_copy().wait_recv()

            @pl.loop(0, EDGE)
            def _(q):
                pair[q] = pair[q] + over_z[q]

            x_copy(pair, 2).start()

        @pl.when(lo == half + 2)
        def _():
            z_copy().wait_recv()
            x_copy(over_z, -2).start()

    def rest_3():
        @pl.when(even & (lo > 0))
        def _():
            x_copy(pair, 2).wait_recv()

        @pl.when(lo == 0)
        def _():
            @pl.loop(0, EDGE)
            def _(q):
                before[q] = zero_row

        @pl.when(even & (lo > 0))
        def _():
            @pl.loop(0, EDGE)
            def _(q):
                before[q] = over_x[q]

        @pl.when(even & (lo >= half))
        def _():
            @pl.loop(0, EDGE)
            def _(q):
                before[q] = before[q] + over_z[q]

        @pl.when(even)
        def _():
            @pl.loop(0, EDGE)
            def _(q):
                through[q] = before[q] + tot[q]

            back_copy().start()

    def edge_0():
        @pl.when(even)
        def _():
            mate_copy(B).start()

    FARS = (3, 1, 2)

    def edge_1():
        @pl.when(odd)
        def _():
            mate_copy(B).wait_recv()
            joint[...] = tot[EDGE] + mate[EDGE]
            for far in FARS:
                @pl.when(lo + 2 * far < lon_size)
                def _():
                    far_copy(far, 1).start()
                    far_copy(far, 0).start()

    def edge_2():
        before[EDGE] = zero_row
        for far in range(1, slots):
            @pl.when(lo >= 2 * far)
            def _():
                far_copy(far, 1).wait_recv()
                before[EDGE] = before[EDGE] + earlier[far - 1]

        @pl.when(odd)
        def _():
            before[EDGE] = before[EDGE] + mate[EDGE]

    def prefix_end():
        @pl.when(odd)
        def _():
            back_copy().wait_recv()
            mate_copy(A).wait_send()
            for far in FARS:
                @pl.when(lo + 2 * far < lon_size)
                def _():
                    far_copy(far, 1).wait_send()
                    far_copy(far, 0).wait_send()

        @pl.when(even)
        def _():
            back_copy().wait_send()
            mate_copy(B).wait_send()

        @pl.when(low_even)
        def _():
            z_copy().wait_send()

        @pl.when(among((0, half, half + 2)))
        def _():
            x_copy(pair, 2).wait_send()

    def send_lat(tick):
        if tick >= CHUNKS:
            lat_copy(tick - CHUNKS).wait_send()
        lat_copy(tick).start()

    load(EDGE).wait()
    send_lat(0)
    send_lat(1)
    for p in (0, 3, 1, 2):
        load_pair(1, p).start()
        load_pair(2, p).start()
    send_lev(0, LAST)
    for side in range(2):
        send_near(0, side)

    @pl.loop(0, N)
    def _(i):
        for b in range(2):
            s[b, 0, i + 1, cells, :] = zero_row

    for side, row in ((0, 0), (1, N + 1)):
        @pl.when(jnp.logical_not(has_lon[side]))
        def _():
            @pl.loop(0, Q)
            def _(q):
                for b in range(2):
                    s[b, q + 1, row, cells, :] = zero_row

    for side, cell in ((0, PAD - 1), (1, TOP)):
        @pl.when(jnp.logical_not(has_lev[side]))
        def _():
            @pl.loop(0, Q)
            def _(q):
                @pl.loop(0, N)
                def _(i):
                    for b in range(2):
                        s[b, q + 1, i + 1, pl.ds(cell, 1), :] = zero_cell

    for g in range(LAST):
        q0, planes = GROUPS[g]
        for q in range(q0, q0 + planes):
            load(q).wait()
        send_lev(0, g)
        send_lon(0, g)
        send_lat(g + 2)

    def update_planes(t, planes):
        for q in planes:
            g = q // 4
            q0, n = GROUPS[g]
            if t == 0 and q % 2 == 0 and q // 2 < 3:
                for array in (1, 2):
                    load_pair(array, q // 2).wait()
            if q == q0:
                arrived_lev(t, g)
                for side in range(2):
                    arrived_lon(t, g, side)
                if t > 0:
                    sent_lev(t - 1, g)
                    sent_lon(t - 1, g)
            update_plane(t, q)
            if t < STEPS - 1 and q == q0 + n - 1:
                send_lev(t + 1, g)
                send_lon(t + 1, g)

    for t in range(STEPS):
        final = t == STEPS - 1
        for n in range(CHUNKS):
            tick = t * CHUNKS + n
            if final and n == 0:
                update_planes(t, range(EDGE))
                rest_0()
            lat_copy(tick).wait_recv()
            if tick + WINDOW < TICKS:
                send_lat(tick + WINDOW)
            if n < 2:
                @pl.when(wide[n])
                def _():
                    turn_copy(t, n).start()
            if t == 0 and n == 1:
                pass_on(0, RELAY[0])
            if not final and n == PASS:
                pass_on(t + 1, RELAY[0])
            for m in LATE.get(n, ()):
                if m == 2:
                    if t == 0:
                        for array in (1, 2):
                            load_pair(array, 3).wait()
                    arrived_lev(t, LAST)
                    if t > 0:
                        sent_lev(t - 1, LAST)
                        sent_lon(t - 1, LAST)
                if m < 2:
                    arrived_lon(t, LAST, 1 - m)

                    @pl.when(wide[m])
                    def _():
                        turn_copy(t, m).wait_send()
                update_chunk(t, m)
                if not final and m < 2:
                    send_near(t + 1, m)
            if not final:
                update_planes(t, [q for q in (2 * n, 2 * n + 1) if q < EDGE])
            if final and n == 2:
                rest_1()
            if final and n == 4:
                rest_2()
        if not final:
            send_lev(t + 1, LAST)
    edge_0()
    edge_1()
    rest_3()
    edge_2()
    for n in range(CHUNKS):
        lat_copy(TICKS - CHUNKS + n).wait_send()
    for g in range(len(GROUPS)):
        sent_lev(STEPS - 1, g)
        sent_lon(STEPS - 1, g)
    for t in (STEPS - 2, STEPS - 1):
        for g in RELAY:
            for side in range(2):
                @pl.when(keeper[side])
                def _():
                    pass_copy(t, g, side).wait_send()
    prefix_end()


def finish(last, before, totals, end, run, t_sem, c_sem):
    la = lax.axis_index("lat")
    scale = 1.0 / (N * lax.axis_size("lon"))

    def place(q):
        return q + la * (Q - 1 - 2 * q)

    def put_end(p):
        planes = pl.ds(p * (Q // PIECES), Q // PIECES)
        return pltpu.make_async_copy(last.at[planes], end.at[planes], t_sem.at[p])

    def put_totals(q):
        return pltpu.make_async_copy(run.at[q], totals.at[place(q)], c_sem.at[q])

    for p in range(PIECES):
        put_end(p).start()
    for q in range(Q):
        def row(i, total):
            total = total + last[place(q), i]
            run[q, i] = total * scale
            return total
        lax.fori_loop(0, N, row, before[q])
        put_totals(q).start()
    for p in range(PIECES):
        put_end(p).wait()
    for q in range(Q):
        put_totals(q).wait()


def per_device(x, d, f):
    hbm = pl.BlockSpec(memory_space=pltpu.HBM)
    vmem = pl.BlockSpec(memory_space=pltpu.VMEM)
    slots = lax.axis_size("lon") // 2
    dma = pltpu.SemaphoreType.DMA
    block = (Q, N, K, M)
    part = (Q, K, M)
    f32 = jnp.float32
    last, before = pl.pallas_call(
        exchange,
        out_shape=(pltpu.VMEM(block, f32), pltpu.VMEM(part, f32)),
        in_specs=[hbm] * 3,
        out_specs=(vmem, vmem),
        scratch_shapes=[
            pltpu.VMEM((2, Q + 2, N + 2, K + 2 * PAD, M), f32),
            pltpu.VMEM(block, f32),
            pltpu.VMEM(block, f32),
            pltpu.VMEM((STEPS, len(RELAY), 3, K, M), f32),
            pltpu.VMEM(part, f32),
            pltpu.VMEM(part, f32),
            pltpu.VMEM((EDGE, K, M), f32),
            pltpu.VMEM((K, M), f32),
            pltpu.VMEM((EDGE, K, M), f32),
            pltpu.VMEM((EDGE, K, M), f32),
            pltpu.VMEM((EDGE, K, M), f32),
            pltpu.VMEM((slots - 1, K, M), f32),
            dma((Q,)), dma((2, Q // 2)),
            dma((CHUNKS,)), dma((CHUNKS,)),
            dma((2, len(GROUPS), 2)), dma((2, len(GROUPS), 2)),
            dma((2, len(GROUPS), 2)), dma((2, len(GROUPS), 2)),
            dma((2, len(RELAY))), dma((2, len(RELAY))), dma,
            dma((2,)), dma((2,)), dma, dma, dma, dma, dma, dma,
            dma((slots - 1, 2)), dma((slots - 1,)),
        ],
        compiler_params=pltpu.CompilerParams(
            collective_id=0, has_side_effects=True, vmem_limit_bytes=52 * 1024 * 1024),
        name="exchange",
    )(x, d, f)
    totals, end = pl.pallas_call(
        finish,
        out_shape=(jax.ShapeDtypeStruct(block, f32), jax.ShapeDtypeStruct(block, f32)),
        in_specs=[vmem, vmem],
        out_specs=(hbm, hbm),
        scratch_shapes=[pltpu.VMEM(block, f32), dma((PIECES,)), dma((Q,))],
        compiler_params=pltpu.CompilerParams(vmem_limit_bytes=16 * 1024 * 1024),
        name="finish",
    )(last, before)
    return totals, end


def solution(mesh):
    spec = P("lat", "lon", "lev", None)
    return jax.shard_map(
        per_device, mesh=mesh, in_specs=(spec,) * 3, out_specs=(spec, spec), check_vma=False)
```

```python
import functools

import jax
import jax.numpy as jnp
from jax import lax
from jax.experimental import pallas as pl
from jax.experimental.pallas import tpu as pltpu
from jax.sharding import PartitionSpec as P

STEPS = 4
MESH = pl.DeviceIdType.MESH
Q, N, K, M = 8, 32, 64, 128
PAD = 8
TOP = PAD + K
EDGE = Q - 1
CHUNKS = 8
ROWS = N // CHUNKS
ORDER = (0, 7, 1, 2, 3, 4, 5, 6)
WINDOW = 4
TICKS = STEPS * CHUNKS
GROUPS = ((0, 4), (4, 3), (7, 1))
LAST = len(GROUPS) - 1
RELAY = (1,)
LATE = {2: (2, 0), 3: (3, 1), 4: (4,), 5: (5,), 6: (6,), 7: (7,)}
PIECES = 4
A, B = 0, 1
PASS = 5
PLANES = ((0, Q - 1), (Q - 1, 1))
GREET = ((1, range(7)), (2, (0, 1, 3, 4, 5)), (3, (0, 1, 3, 4)), (4, (0, 1, 2, 3)), (5, (1,)), (6, (1,)))


def exchange(*refs):
    dma = pltpu.SemaphoreType.DMA
    groups, slots = len(GROUPS), lax.axis_size("lon") // 2
    own = (dma((Q,)), dma((2, Q // 2)), dma((CHUNKS,)), dma((2, groups, 2)), dma((2, groups, 2)),
           dma((2, len(RELAY))), dma, dma((2,)), dma, dma, dma, dma((slots - 1, 2)),
           dma((CHUNKS,)), dma((2, groups, 2)), dma((2, groups, 2)), dma((2, len(RELAY))),
           dma((2,)), dma, dma, dma, dma((slots - 1,)))
    pl.run_scoped(functools.partial(exchange_with, refs), *own)


def exchange_with(refs, in_sem, pair_sem, lat_s, lon_s, lev_s, hold_s, turn_s, mate_s, z_s, x_s, back_s, far_s,
                  lat_r, lon_r, lev_r, hold_r, mate_r, z_r, x_r, back_r, far_r):
    (x, d, f, last, before, s, dv, fv, hold, tot, mate, pair, joint, over_z, over_x, through, earlier) = refs
    la, lo, le = lax.axis_index("lat"), lax.axis_index("lon"), lax.axis_index("lev")
    lon_size, lev_size = lax.axis_size("lon"), lax.axis_size("lev")
    half = lon_size // 2
    has_lon = (lo > 0, lo < lon_size - 1)
    has_lev = (le > 0, le < lev_size - 1)
    odd = lo % 2 == 1
    even = lo % 2 == 0
    near = (odd, even)
    wide = (even & (lo > 0), odd & (lo < lon_size - 1))
    slots = lon_size // 2
    cells = pl.ds(PAD, K)

    def place(q):
        return q + la * (Q - 1 - 2 * q)

    def load(q):
        return pltpu.make_async_copy(x.at[place(q)], s.at[0, q + 1, pl.ds(1, N), cells, :], in_sem.at[q])

    def load_pair(n, p):
        planes = pl.ds(2 * p + la * (Q - 2 - 4 * p), 2)
        return pltpu.make_async_copy((d, f)[n - 1].at[planes], (dv, fv)[n - 1].at[planes], pair_sem.at[n - 1, p])

    load(EDGE).start()

    barrier = pltpu.get_barrier_semaphore()

    def greet(dev):
        pl.semaphore_signal(barrier, inc=1, device_id=dev, device_id_type=MESH)

    def among(members):
        found = lo < 0
        for m in members:
            found = found | (lo == m)
        return found

    greet((1 - la, lo, le))
    count = jnp.int32(1)
    peers = [
        (has_lev[0], (la, lo, le - 1)),
        (has_lev[1], (la, lo, le + 1)),
        (wide[0], (1 - la, lo - 1, le)),
        (wide[1], (1 - la, lo + 1, le)),
    ]
    for offset, lower in GREET:
        peers.append((among(lower), (la, lo + offset, le)))
        peers.append((among([m + offset for m in lower]), (la, lo - offset, le)))
    for there, dev in peers:
        count = count + there.astype(jnp.int32)

        @pl.when(there)
        def _():
            greet(dev)

    for q in range(EDGE):
        load(q).start()
    pl.semaphore_wait(barrier, count)

    zero_row = jnp.zeros((K, M), jnp.float32)
    zero_cell = jnp.zeros((1, M), jnp.float32)

    def lat_copy(tick):
        t, c = tick // CHUNKS, ORDER[tick % CHUNKS]
        rows = pl.ds(1 + c * ROWS, ROWS)
        return pltpu.make_async_remote_copy(
            src_ref=s.at[t % 2, Q, rows, cells, :],
            dst_ref=s.at[t % 2, Q + 1, rows, cells, :],
            send_sem=lat_s.at[tick % CHUNKS], recv_sem=lat_r.at[tick % CHUNKS],
            device_id=(1 - la, lo, le), device_id_type=MESH)

    FROM, TO = (1, N), (N + 1, 0)

    def face(t, g, i):
        q, n = GROUPS[g]
        return s.at[t % 2, pl.ds(q + 1, n), i, cells, :]

    def lon_copy(t, g, side):
        return pltpu.make_async_remote_copy(
            src_ref=face(t, g, FROM[side]), dst_ref=face(t, g, TO[side]),
            send_sem=lon_s.at[t % 2, g, side], recv_sem=lon_r.at[t % 2, g, side],
            device_id=(la, lo + (-1, 1)[side], le), device_id_type=MESH)

    def held(t, g):
        r = RELAY.index(g)
        return hold.at[t, r, pl.ds(0, GROUPS[g][1])], t % 2, r

    def hold_copy(t, g, side):
        buffer, b, r = held(t, g)
        return pltpu.make_async_remote_copy(
            src_ref=face(t, g, FROM[side]), dst_ref=buffer,
            send_sem=lon_s.at[b, g, side], recv_sem=hold_r.at[b, r],
            device_id=(la, lo + (-half, half)[side], le), device_id_type=MESH)

    def pass_copy(t, g, side):
        buffer, b, r = held(t, g)
        return pltpu.make_async_remote_copy(
            src_ref=buffer, dst_ref=face(t, g, TO[side]),
            send_sem=hold_s.at[b, r], recv_sem=lon_r.at[b, g, side],
            device_id=(la, lo + (half - 1, 1 - half)[side], le), device_id_type=MESH)

    def turn_copy(t, side):
        return pltpu.make_async_remote_copy(
            src_ref=s.at[t % 2, Q + 1, FROM[side], cells, :],
            dst_ref=s.at[t % 2, Q, TO[side], cells, :],
            send_sem=turn_s, recv_sem=lon_r.at[t % 2, LAST, side],
            device_id=(1 - la, lo + (-1, 1)[side], le), device_id_type=MESH)

    def lev_copy(t, g, side):
        q, n = GROUPS[g]
        planes = pl.ds(q + 1, n)
        return pltpu.make_async_remote_copy(
            src_ref=s.at[t % 2, planes, pl.ds(1, N), pl.ds((PAD, TOP - 1)[side], 1), :],
            dst_ref=s.at[t % 2, planes, pl.ds(1, N), pl.ds((TOP, PAD - 1)[side], 1), :],
            send_sem=lev_s.at[t % 2, g, side], recv_sem=lev_r.at[t % 2, g, side],
            device_id=(la, lo, le + (-1, 1)[side]), device_id_type=MESH)

    sender = (lo == half, lo == half - 1)
    keeper = (lo == 0, lo == lon_size - 1)

    def send_lev(t, q):
        for side in range(2):
            @pl.when(has_lev[side])
            def _():
                lev_copy(t, q, side).start()

    def send_lon(t, q):
        for side in range(2):
            if q in RELAY:
                @pl.when(has_lon[side] & jnp.logical_not(sender[side]))
                def _():
                    lon_copy(t, q, side).start()

                @pl.when(sender[side])
                def _():
                    hold_copy(t, q, side).start()
            else:
                @pl.when(has_lon[side])
                def _():
                    lon_copy(t, q, side).start()

    def send_near(t, side):
        @pl.when(near[side])
        def _():
            lon_copy(t, LAST, side).start()

    def pass_on(t, q):
        for side in range(2):
            @pl.when(keeper[side])
            def _():
                if t > 1:
                    pass_copy(t - 2, q, side).wait_send()
                hold_copy(t, q, side).wait_recv()
                pass_copy(t, q, side).start()

    def sent_lev(t, q):
        for side in range(2):
            @pl.when(has_lev[side])
            def _():
                lev_copy(t, q, side).wait_send()

    def sent_lon(t, q):
        for side in range(2):
            @pl.when(near[side] if q == LAST else has_lon[side])
            def _():
                lon_copy(t, q, side).wait_send()

    def arrived_lev(t, q):
        for side in range(2):
            @pl.when(has_lev[1 - side])
            def _():
                lev_copy(t, q, side).wait_recv()

    def arrived_lon(t, q, side):
        @pl.when(has_lon[1 - side])
        def _():
            lon_copy(t, q, side).wait_recv()

    def update(t, q, i):
        b = t % 2
        here = s.at[b, q + 1, i + 1]
        middle = here[cells, :]
        spread = here[pl.ds(PAD - 1, K), :] + here[pl.ds(PAD + 1, K), :]
        spread += s[b, q + 1, i, cells, :] + s[b, q + 1, i + 2, cells, :]
        spread += s[b, q, i + 1, cells, :] + s[b, q + 2, i + 1, cells, :]
        j = place(q)
        new = middle + dv[j, i] * (spread - 6.0 * middle) + fv[j, i]
        if t == STEPS - 1:
            last[j, i] = new
        else:
            s[1 - b, q + 1, i + 1, cells, :] = new
        return new

    def update_plane(t, q):
        if t == STEPS - 1:
            def add(i, total):
                return total + update(t, q, i)
            tot[q] = lax.fori_loop(0, N, add, zero_row)
        else:
            @pl.loop(0, N)
            def _(i):
                update(t, q, i)

    def update_chunk(t, n):
        c = ORDER[n]
        if t == STEPS - 1:
            def add(i, total):
                return total + update(t, EDGE, i)
            total = lax.fori_loop(c * ROWS, (c + 1) * ROWS, add, zero_row)
            if n == LATE[2][0]:
                tot[EDGE] = total
            else:
                tot[EDGE] = tot[EDGE] + total
        else:
            @pl.loop(c * ROWS, (c + 1) * ROWS)
            def _(i):
                update(t, EDGE, i)

    def mate_copy(group):
        planes = pl.ds(*PLANES[group])
        return pltpu.make_async_remote_copy(
            src_ref=tot.at[planes], dst_ref=mate.at[planes],
            send_sem=mate_s.at[group], recv_sem=mate_r.at[group],
            device_id=(la, lo + (-1, 1)[group], le), device_id_type=MESH)

    rest = pl.ds(*PLANES[A])

    def z_copy():
        return pltpu.make_async_remote_copy(
            src_ref=pair, dst_ref=over_z, send_sem=z_s, recv_sem=z_r,
            device_id=(la, lo + half, le), device_id_type=MESH)

    def x_copy(source, offset):
        return pltpu.make_async_remote_copy(
            src_ref=source, dst_ref=over_x, send_sem=x_s, recv_sem=x_r,
            device_id=(la, lo + offset, le), device_id_type=MESH)

    def back_copy():
        return pltpu.make_async_remote_copy(
            src_ref=through, dst_ref=before.at[rest], send_sem=back_s, recv_sem=back_r,
            device_id=(la, lo + 1, le), device_id_type=MESH)

    def far_copy(far, to_odd):
        return pltpu.make_async_remote_copy(
            src_ref=joint, dst_ref=earlier.at[far - 1],
            send_sem=far_s.at[far - 1, to_odd], recv_sem=far_r.at[far - 1],
            device_id=(la, lo + 2 * far - 1 + to_odd, le), device_id_type=MESH)

    low_even = even & (lo < half)

    def rest_0():
        @pl.when(odd)
        def _():
            mate_copy(A).start()

    def rest_1():
        @pl.when(even)
        def _():
            mate_copy(A).wait_recv()

            @pl.loop(0, EDGE)
            def _(q):
                pair[q] = tot[q] + mate[q]

        @pl.when(lo == 0)
        def _():
            x_copy(pair, 2).start()

        @pl.when(low_even)
        def _():
            z_copy().start()

    def rest_2():
        @pl.when(lo == half)
        def _():
            z_copy().wait_recv()

            @pl.loop(0, EDGE)
            def _(q):
                pair[q] = pair[q] + over_z[q]

            x_copy(pair, 2).start()

        @pl.when(lo == half + 2)
        def _():
            z_copy().wait_recv()
            x_copy(over_z, -2).start()

    def rest_3():
        @pl.when(even & (lo > 0))
        def _():
            x_copy(pair, 2).wait_recv()

        @pl.when(lo == 0)
        def _():
            @pl.loop(0, EDGE)
            def _(q):
                before[q] = zero_row

        @pl.when(even & (lo > 0))
        def _():
            @pl.loop(0, EDGE)
            def _(q):
                before[q] = over_x[q]

        @pl.when(even & (lo >= half))
        def _():
            @pl.loop(0, EDGE)
            def _(q):
                before[q] = before[q] + over_z[q]

        @pl.when(even)
        def _():
            @pl.loop(0, EDGE)
            def _(q):
                through[q] = before[q] + tot[q]

            back_copy().start()

    def edge_0():
        @pl.when(even)
        def _():
            mate_copy(B).start()

    FARS = (3, 1, 2)

    def edge_1():
        @pl.when(odd)
        def _():
            mate_copy(B).wait_recv()
            joint[...] = tot[EDGE] + mate[EDGE]
            for far in FARS:
                @pl.when(lo + 2 * far < lon_size)
                def _():
                    far_copy(far, 1).start()
                    far_copy(far, 0).start()

    def edge_2():
        before[EDGE] = zero_row
        for far in range(1, slots):
            @pl.when(lo >= 2 * far)
            def _():
                far_copy(far, 1).wait_recv()
                before[EDGE] = before[EDGE] + earlier[far - 1]

        @pl.when(odd)
        def _():
            before[EDGE] = before[EDGE] + mate[EDGE]

    def prefix_end():
        @pl.when(odd)
        def _():
            back_copy().wait_recv()
            mate_copy(A).wait_send()
            for far in FARS:
                @pl.when(lo + 2 * far < lon_size)
                def _():
                    far_copy(far, 1).wait_send()
                    far_copy(far, 0).wait_send()

        @pl.when(even)
        def _():
            back_copy().wait_send()
            mate_copy(B).wait_send()

        @pl.when(low_even)
        def _():
            z_copy().wait_send()

        @pl.when(among((0, half, half + 2)))
        def _():
            x_copy(pair, 2).wait_send()

    def send_lat(tick):
        if tick >= CHUNKS:
            lat_copy(tick - CHUNKS).wait_send()
        lat_copy(tick).start()

    load(EDGE).wait()
    send_lat(0)
    send_lat(1)
    for p in (0, 3, 1, 2):
        load_pair(1, p).start()
        load_pair(2, p).start()
    send_lev(0, LAST)
    for side in range(2):
        send_near(0, side)

    @pl.loop(0, N)
    def _(i):
        for b in range(2):
            s[b, 0, i + 1, cells, :] = zero_row

    for side, row in ((0, 0), (1, N + 1)):
        @pl.when(jnp.logical_not(has_lon[side]))
        def _():
            @pl.loop(0, Q)
            def _(q):
                for b in range(2):
                    s[b, q + 1, row, cells, :] = zero_row

    for side, cell in ((0, PAD - 1), (1, TOP)):
        @pl.when(jnp.logical_not(has_lev[side]))
        def _():
            @pl.loop(0, Q)
            def _(q):
                @pl.loop(0, N)
                def _(i):
                    for b in range(2):
                        s[b, q + 1, i + 1, pl.ds(cell, 1), :] = zero_cell

    for g in range(LAST):
        q0, planes = GROUPS[g]
        for q in range(q0, q0 + planes):
            load(q).wait()
        send_lev(0, g)
        send_lon(0, g)
        send_lat(g + 2)

    def update_planes(t, planes):
        for q in planes:
            g = q // 4
            q0, n = GROUPS[g]
            if t == 0 and q % 2 == 0 and q // 2 < 3:
                for array in (1, 2):
                    load_pair(array, q // 2).wait()
            if q == q0:
                arrived_lev(t, g)
                for side in range(2):
                    arrived_lon(t, g, side)
                if t > 0:
                    sent_lev(t - 1, g)
                    sent_lon(t - 1, g)
            update_plane(t, q)
            if t < STEPS - 1 and q == q0 + n - 1:
                send_lev(t + 1, g)
                send_lon(t + 1, g)

    for t in range(STEPS):
        final = t == STEPS - 1
        for n in range(CHUNKS):
            tick = t * CHUNKS + n
            if final and n == 0:
                update_planes(t, range(EDGE))
                rest_0()
            lat_copy(tick).wait_recv()
            if tick + WINDOW < TICKS:
                send_lat(tick + WINDOW)
            if n < 2:
                @pl.when(wide[n])
                def _():
                    turn_copy(t, n).start()
            if t == 0 and n == 1:
                pass_on(0, RELAY[0])
            if not final and n == PASS:
                pass_on(t + 1, RELAY[0])
            for m in LATE.get(n, ()):
                if m == 2:
                    if t == 0:
                        for array in (1, 2):
                            load_pair(array, 3).wait()
                    arrived_lev(t, LAST)
                    if t > 0:
                        sent_lev(t - 1, LAST)
                        sent_lon(t - 1, LAST)
                if m < 2:
                    arrived_lon(t, LAST, 1 - m)

                    @pl.when(wide[m])
                    def _():
                        turn_copy(t, m).wait_send()
                update_chunk(t, m)
                if not final and m < 2:
                    send_near(t + 1, m)
            if not final:
                update_planes(t, [q for q in (2 * n, 2 * n + 1) if q < EDGE])
            if final and n == 2:
                rest_1()
            if final and n == 4:
                rest_2()
        if not final:
            send_lev(t + 1, LAST)
    edge_0()
    edge_1()
    rest_3()
    edge_2()
    for n in range(CHUNKS):
        lat_copy(TICKS - CHUNKS + n).wait_send()
    for g in range(len(GROUPS)):
        sent_lev(STEPS - 1, g)
        sent_lon(STEPS - 1, g)
    for t in (STEPS - 2, STEPS - 1):
        for g in RELAY:
            for side in range(2):
                @pl.when(keeper[side])
                def _():
                    pass_copy(t, g, side).wait_send()
    prefix_end()


def finish(*refs):
    dma = pltpu.SemaphoreType.DMA
    pl.run_scoped(functools.partial(finish_with, *refs), dma((PIECES,)), dma((Q,)))


def finish_with(last, before, totals, end, run, t_sem, c_sem):
    la = lax.axis_index("lat")
    scale = 1.0 / (N * lax.axis_size("lon"))

    def place(q):
        return q + la * (Q - 1 - 2 * q)

    def put_end(p):
        planes = pl.ds(p * (Q // PIECES), Q // PIECES)
        return pltpu.make_async_copy(last.at[planes], end.at[planes], t_sem.at[p])

    def put_totals(q):
        return pltpu.make_async_copy(run.at[q], totals.at[place(q)], c_sem.at[q])

    for p in range(PIECES):
        put_end(p).start()
    for q in range(Q):
        def row(i, total):
            total = total + last[place(q), i]
            run[q, i] = total * scale
            return total
        lax.fori_loop(0, N, row, before[q])
        put_totals(q).start()
    for p in range(PIECES):
        put_end(p).wait()
    for q in range(Q):
        put_totals(q).wait()


def per_device(x, d, f):
    hbm = pl.BlockSpec(memory_space=pltpu.HBM)
    vmem = pl.BlockSpec(memory_space=pltpu.VMEM)
    slots = lax.axis_size("lon") // 2
    block = (Q, N, K, M)
    part = (Q, K, M)
    f32 = jnp.float32
    last, before = pl.pallas_call(
        exchange,
        out_shape=(pltpu.VMEM(block, f32), pltpu.VMEM(part, f32)),
        in_specs=[hbm] * 3,
        out_specs=(vmem, vmem),
        scratch_shapes=[
            pltpu.VMEM((2, Q + 2, N + 2, K + 2 * PAD, M), f32),
            pltpu.VMEM(block, f32),
            pltpu.VMEM(block, f32),
            pltpu.VMEM((STEPS, len(RELAY), 3, K, M), f32),
            pltpu.VMEM(part, f32),
            pltpu.VMEM(part, f32),
            pltpu.VMEM((EDGE, K, M), f32),
            pltpu.VMEM((K, M), f32),
            pltpu.VMEM((EDGE, K, M), f32),
            pltpu.VMEM((EDGE, K, M), f32),
            pltpu.VMEM((EDGE, K, M), f32),
            pltpu.VMEM((slots - 1, K, M), f32),
        ],
        compiler_params=pltpu.CompilerParams(
            collective_id=0, has_side_effects=True, vmem_limit_bytes=52 * 1024 * 1024),
        name="exchange",
    )(x, d, f)
    totals, end = pl.pallas_call(
        finish,
        out_shape=(jax.ShapeDtypeStruct(block, f32), jax.ShapeDtypeStruct(block, f32)),
        in_specs=[vmem, vmem],
        out_specs=(hbm, hbm),
        scratch_shapes=[pltpu.VMEM(block, f32)],
        compiler_params=pltpu.CompilerParams(vmem_limit_bytes=16 * 1024 * 1024),
        name="finish",
    )(last, before)
    return totals, end


def solution(mesh):
    spec = P("lat", "lon", "lev", None)
    return jax.shard_map(
        per_device, mesh=mesh, in_specs=(spec,) * 3, out_specs=(spec, spec), check_vma=False)
```

```python
import functools

import jax
import jax.numpy as jnp
from jax import lax
from jax.experimental import pallas as pl
from jax.experimental.pallas import tpu as pltpu
from jax.sharding import PartitionSpec as P

STEPS = 4
MESH = pl.DeviceIdType.MESH
Q, N, K, M = 8, 32, 64, 128
PAD = 8
TOP = PAD + K
EDGE = Q - 1
CHUNKS = 8
ROWS = N // CHUNKS
ORDER = (0, 7, 1, 2, 3, 4, 5, 6)
WINDOW = 5
TICKS = STEPS * CHUNKS
GROUPS = ((0, 4), (4, 3), (7, 1))
LAST = len(GROUPS) - 1
RELAY = (1,)
LATE = {2: (2, 0), 3: (3, 1), 4: (4,), 5: (5,), 6: (6,), 7: (7,)}
PIECES = 4
A, B = 0, 1
PASS = 5
PLANES = ((0, Q - 1), (Q - 1, 1))
GREET = ((1, range(7)), (2, (0, 1, 3, 4, 5)), (3, (0, 1, 3, 4)), (4, (0, 1, 2, 3)), (5, (1,)), (6, (1,)))


def exchange(*refs):
    dma = pltpu.SemaphoreType.DMA
    groups, slots = len(GROUPS), lax.axis_size("lon") // 2
    own = (dma((Q,)), dma((2, Q // 2)), dma((TICKS,)), dma((2, groups, 2)), dma((2, groups, 2)),
           dma((2, len(RELAY))), dma, dma((2,)), dma, dma, dma, dma((slots - 1, 2)),
           dma((TICKS,)), dma((2, groups, 2)), dma((2, groups, 2)), dma((2, len(RELAY))),
           dma((2,)), dma, dma, dma, dma((slots - 1,)))
    pl.run_scoped(functools.partial(exchange_with, refs), *own)


def exchange_with(refs, in_sem, pair_sem, lat_s, lon_s, lev_s, hold_s, turn_s, mate_s, z_s, x_s, back_s, far_s,
                  lat_r, lon_r, lev_r, hold_r, mate_r, z_r, x_r, back_r, far_r):
    (x, d, f, last, before, s, dv, fv, hold, tot, mate, pair, joint, over_z, over_x, through, earlier) = refs
    la, lo, le = lax.axis_index("lat"), lax.axis_index("lon"), lax.axis_index("lev")
    lon_size, lev_size = lax.axis_size("lon"), lax.axis_size("lev")
    half = lon_size // 2
    has_lon = (lo > 0, lo < lon_size - 1)
    has_lev = (le > 0, le < lev_size - 1)
    odd = lo % 2 == 1
    even = lo % 2 == 0
    near = (odd, even)
    wide = (even & (lo > 0), odd & (lo < lon_size - 1))
    slots = lon_size // 2
    cells = pl.ds(PAD, K)

    def place(q):
        return q + la * (Q - 1 - 2 * q)

    def load(q):
        return pltpu.make_async_copy(x.at[place(q)], s.at[0, q + 1, pl.ds(1, N), cells, :], in_sem.at[q])

    def load_pair(n, p):
        planes = pl.ds(2 * p + la * (Q - 2 - 4 * p), 2)
        return pltpu.make_async_copy((d, f)[n - 1].at[planes], (dv, fv)[n - 1].at[planes], pair_sem.at[n - 1, p])

    load(EDGE).start()

    barrier = pltpu.get_barrier_semaphore()

    def greet(dev):
        pl.semaphore_signal(barrier, inc=1, device_id=dev, device_id_type=MESH)

    def among(members):
        found = lo < 0
        for m in members:
            found = found | (lo == m)
        return found

    greet((1 - la, lo, le))
    count = jnp.int32(1)
    peers = [
        (has_lev[0], (la, lo, le - 1)),
        (has_lev[1], (la, lo, le + 1)),
        (wide[0], (1 - la, lo - 1, le)),
        (wide[1], (1 - la, lo + 1, le)),
    ]
    for offset, lower in GREET:
        peers.append((among(lower), (la, lo + offset, le)))
        peers.append((among([m + offset for m in lower]), (la, lo - offset, le)))
    for there, dev in peers:
        count = count + there.astype(jnp.int32)

        @pl.when(there)
        def _():
            greet(dev)

    for q in range(EDGE):
        load(q).start()
    pl.semaphore_wait(barrier, count)

    zero_row = jnp.zeros((K, M), jnp.float32)
    zero_cell = jnp.zeros((1, M), jnp.float32)

    def lat_copy(tick):
        t, c = tick // CHUNKS, ORDER[tick % CHUNKS]
        rows = pl.ds(1 + c * ROWS, ROWS)
        return pltpu.make_async_remote_copy(
            src_ref=s.at[t % 2, Q, rows, cells, :],
            dst_ref=s.at[t % 2, Q + 1, rows, cells, :],
            send_sem=lat_s.at[tick], recv_sem=lat_r.at[tick],
            device_id=(1 - la, lo, le), device_id_type=MESH)

    FROM, TO = (1, N), (N + 1, 0)

    def face(t, g, i):
        q, n = GROUPS[g]
        return s.at[t % 2, pl.ds(q + 1, n), i, cells, :]

    def lon_copy(t, g, side):
        return pltpu.make_async_remote_copy(
            src_ref=face(t, g, FROM[side]), dst_ref=face(t, g, TO[side]),
            send_sem=lon_s.at[t % 2, g, side], recv_sem=lon_r.at[t % 2, g, side],
            device_id=(la, lo + (-1, 1)[side], le), device_id_type=MESH)

    def held(t, g):
        r = RELAY.index(g)
        return hold.at[t, r, pl.ds(0, GROUPS[g][1])], t % 2, r

    def hold_copy(t, g, side):
        buffer, b, r = held(t, g)
        return pltpu.make_async_remote_copy(
            src_ref=face(t, g, FROM[side]), dst_ref=buffer,
            send_sem=lon_s.at[b, g, side], recv_sem=hold_r.at[b, r],
            device_id=(la, lo + (-half, half)[side], le), device_id_type=MESH)

    def pass_copy(t, g, side):
        buffer, b, r = held(t, g)
        return pltpu.make_async_remote_copy(
            src_ref=buffer, dst_ref=face(t, g, TO[side]),
            send_sem=hold_s.at[b, r], recv_sem=lon_r.at[b, g, side],
            device_id=(la, lo + (half - 1, 1 - half)[side], le), device_id_type=MESH)

    def turn_copy(t, side):
        return pltpu.make_async_remote_copy(
            src_ref=s.at[t % 2, Q + 1, FROM[side], cells, :],
            dst_ref=s.at[t % 2, Q, TO[side], cells, :],
            send_sem=turn_s, recv_sem=lon_r.at[t % 2, LAST, side],
            device_id=(1 - la, lo + (-1, 1)[side], le), device_id_type=MESH)

    def lev_copy(t, g, side):
        q, n = GROUPS[g]
        planes = pl.ds(q + 1, n)
        return pltpu.make_async_remote_copy(
            src_ref=s.at[t % 2, planes, pl.ds(1, N), pl.ds((PAD, TOP - 1)[side], 1), :],
            dst_ref=s.at[t % 2, planes, pl.ds(1, N), pl.ds((TOP, PAD - 1)[side], 1), :],
            send_sem=lev_s.at[t % 2, g, side], recv_sem=lev_r.at[t % 2, g, side],
            device_id=(la, lo, le + (-1, 1)[side]), device_id_type=MESH)

    sender = (lo == half, lo == half - 1)
    keeper = (lo == 0, lo == lon_size - 1)

    def send_lev(t, q):
        for side in range(2):
            @pl.when(has_lev[side])
            def _():
                lev_copy(t, q, side).start()

    def send_lon(t, q):
        for side in range(2):
            if q in RELAY:
                @pl.when(has_lon[side] & jnp.logical_not(sender[side]))
                def _():
                    lon_copy(t, q, side).start()

                @pl.when(sender[side])
                def _():
                    hold_copy(t, q, side).start()
            else:
                @pl.when(has_lon[side])
                def _():
                    lon_copy(t, q, side).start()

    def send_near(t, side):
        @pl.when(near[side])
        def _():
            lon_copy(t, LAST, side).start()

    def pass_on(t, q):
        for side in range(2):
            @pl.when(keeper[side])
            def _():
                if t > 1:
                    pass_copy(t - 2, q, side).wait_send()
                hold_copy(t, q, side).wait_recv()
                pass_copy(t, q, side).start()

    def sent_lev(t, q):
        for side in range(2):
            @pl.when(has_lev[side])
            def _():
                lev_copy(t, q, side).wait_send()

    def sent_lon(t, q):
        for side in range(2):
            @pl.when(near[side] if q == LAST else has_lon[side])
            def _():
                lon_copy(t, q, side).wait_send()

    def arrived_lev(t, q):
        for side in range(2):
            @pl.when(has_lev[1 - side])
            def _():
                lev_copy(t, q, side).wait_recv()

    def arrived_lon(t, q, side):
        @pl.when(has_lon[1 - side])
        def _():
            lon_copy(t, q, side).wait_recv()

    def update(t, q, i):
        b = t % 2
        here = s.at[b, q + 1, i + 1]
        middle = here[cells, :]
        spread = here[pl.ds(PAD - 1, K), :] + here[pl.ds(PAD + 1, K), :]
        spread += s[b, q + 1, i, cells, :] + s[b, q + 1, i + 2, cells, :]
        spread += s[b, q, i + 1, cells, :] + s[b, q + 2, i + 1, cells, :]
        j = place(q)
        new = middle + dv[j, i] * (spread - 6.0 * middle) + fv[j, i]
        if t == STEPS - 1:
            last[j, i] = new
        else:
            s[1 - b, q + 1, i + 1, cells, :] = new
        return new

    def update_plane(t, q):
        if t == STEPS - 1:
            def add(i, total):
                return total + update(t, q, i)
            tot[q] = lax.fori_loop(0, N, add, zero_row)
        else:
            @pl.loop(0, N)
            def _(i):
                update(t, q, i)

    def update_chunk(t, n):
        c = ORDER[n]
        if t == STEPS - 1:
            def add(i, total):
                return total + update(t, EDGE, i)
            total = lax.fori_loop(c * ROWS, (c + 1) * ROWS, add, zero_row)
            if n == LATE[2][0]:
                tot[EDGE] = total
            else:
                tot[EDGE] = tot[EDGE] + total
        else:
            @pl.loop(c * ROWS, (c + 1) * ROWS)
            def _(i):
                update(t, EDGE, i)

    def mate_copy(group):
        planes = pl.ds(*PLANES[group])
        return pltpu.make_async_remote_copy(
            src_ref=tot.at[planes], dst_ref=mate.at[planes],
            send_sem=mate_s.at[group], recv_sem=mate_r.at[group],
            device_id=(la, lo + (-1, 1)[group], le), device_id_type=MESH)

    rest = pl.ds(*PLANES[A])

    def z_copy():
        return pltpu.make_async_remote_copy(
            src_ref=pair, dst_ref=over_z, send_sem=z_s, recv_sem=z_r,
            device_id=(la, lo + half, le), device_id_type=MESH)

    def x_copy(source, offset):
        return pltpu.make_async_remote_copy(
            src_ref=source, dst_ref=over_x, send_sem=x_s, recv_sem=x_r,
            device_id=(la, lo + offset, le), device_id_type=MESH)

    def back_copy():
        return pltpu.make_async_remote_copy(
            src_ref=through, dst_ref=before.at[rest], send_sem=back_s, recv_sem=back_r,
            device_id=(la, lo + 1, le), device_id_type=MESH)

    def far_copy(far, to_odd):
        return pltpu.make_async_remote_copy(
            src_ref=joint, dst_ref=earlier.at[far - 1],
            send_sem=far_s.at[far - 1, to_odd], recv_sem=far_r.at[far - 1],
            device_id=(la, lo + 2 * far - 1 + to_odd, le), device_id_type=MESH)

    low_even = even & (lo < half)

    def rest_0():
        @pl.when(odd)
        def _():
            mate_copy(A).start()

    def rest_1():
        @pl.when(even)
        def _():
            mate_copy(A).wait_recv()

            @pl.loop(0, EDGE)
            def _(q):
                pair[q] = tot[q] + mate[q]

        @pl.when(lo == 0)
        def _():
            x_copy(pair, 2).start()

        @pl.when(low_even)
        def _():
            z_copy().start()

    def rest_2():
        @pl.when(lo == half)
        def _():
            z_copy().wait_recv()

            @pl.loop(0, EDGE)
            def _(q):
                pair[q] = pair[q] + over_z[q]

            x_copy(pair, 2).start()

        @pl.when(lo == half + 2)
        def _():
            z_copy().wait_recv()
            x_copy(over_z, -2).start()

    def rest_3():
        @pl.when(even & (lo > 0))
        def _():
            x_copy(pair, 2).wait_recv()

        @pl.when(lo == 0)
        def _():
            @pl.loop(0, EDGE)
            def _(q):
                before[q] = zero_row

        @pl.when(even & (lo > 0))
        def _():
            @pl.loop(0, EDGE)
            def _(q):
                before[q] = over_x[q]

        @pl.when(even & (lo >= half))
        def _():
            @pl.loop(0, EDGE)
            def _(q):
                before[q] = before[q] + over_z[q]

        @pl.when(even)
        def _():
            @pl.loop(0, EDGE)
            def _(q):
                through[q] = before[q] + tot[q]

            back_copy().start()

    def edge_0():
        @pl.when(even)
        def _():
            mate_copy(B).start()

    FARS = (3, 1, 2)

    def edge_1():
        @pl.when(odd)
        def _():
            mate_copy(B).wait_recv()
            joint[...] = tot[EDGE] + mate[EDGE]
            for far in FARS:
                @pl.when(lo + 2 * far < lon_size)
                def _():
                    far_copy(far, 1).start()
                    far_copy(far, 0).start()

    def edge_2():
        before[EDGE] = zero_row
        for far in range(1, slots):
            @pl.when(lo >= 2 * far)
            def _():
                far_copy(far, 1).wait_recv()
                before[EDGE] = before[EDGE] + earlier[far - 1]

        @pl.when(odd)
        def _():
            before[EDGE] = before[EDGE] + mate[EDGE]

    def prefix_end():
        @pl.when(odd)
        def _():
            back_copy().wait_recv()
            mate_copy(A).wait_send()
            for far in FARS:
                @pl.when(lo + 2 * far < lon_size)
                def _():
                    far_copy(far, 1).wait_send()
                    far_copy(far, 0).wait_send()

        @pl.when(even)
        def _():
            back_copy().wait_send()
            mate_copy(B).wait_send()

        @pl.when(low_even)
        def _():
            z_copy().wait_send()

        @pl.when(among((0, half, half + 2)))
        def _():
            x_copy(pair, 2).wait_send()

    def send_lat(tick):
        if tick >= CHUNKS:
            lat_copy(tick - CHUNKS).wait_send()
        lat_copy(tick).start()

    load(EDGE).wait()
    send_lat(0)
    send_lat(1)
    for p in (0, 3, 1, 2):
        load_pair(1, p).start()
        load_pair(2, p).start()
    send_lev(0, LAST)
    for side in range(2):
        send_near(0, side)

    @pl.loop(0, N)
    def _(i):
        for b in range(2):
            s[b, 0, i + 1, cells, :] = zero_row

    for side, row in ((0, 0), (1, N + 1)):
        @pl.when(jnp.logical_not(has_lon[side]))
        def _():
            @pl.loop(0, Q)
            def _(q):
                for b in range(2):
                    s[b, q + 1, row, cells, :] = zero_row

    for side, cell in ((0, PAD - 1), (1, TOP)):
        @pl.when(jnp.logical_not(has_lev[side]))
        def _():
            @pl.loop(0, Q)
            def _(q):
                @pl.loop(0, N)
                def _(i):
                    for b in range(2):
                        s[b, q + 1, i + 1, pl.ds(cell, 1), :] = zero_cell

    for g in range(LAST):
        q0, planes = GROUPS[g]
        for q in range(q0, q0 + planes):
            load(q).wait()
        send_lev(0, g)
        send_lon(0, g)
        send_lat(g + 2)
    for tick in range(4, WINDOW):
        send_lat(tick)

    def update_planes(t, planes):
        for q in planes:
            g = q // 4
            q0, n = GROUPS[g]
            if t == 0 and q % 2 == 0 and q // 2 < 3:
                for array in (1, 2):
                    load_pair(array, q // 2).wait()
            if q == q0:
                arrived_lev(t, g)
                for side in range(2):
                    arrived_lon(t, g, side)
                if t > 0:
                    sent_lev(t - 1, g)
                    sent_lon(t - 1, g)
            update_plane(t, q)
            if t < STEPS - 1 and q == q0 + n - 1:
                send_lev(t + 1, g)
                send_lon(t + 1, g)

    for t in range(STEPS):
        final = t == STEPS - 1
        for n in range(CHUNKS):
            tick = t * CHUNKS + n
            if final and n == 0:
                update_planes(t, range(EDGE))
                rest_0()
            lat_copy(tick).wait_recv()
            if tick + WINDOW < TICKS:
                send_lat(tick + WINDOW)
            if n < 2:
                @pl.when(wide[n])
                def _():
                    turn_copy(t, n).start()
            if t == 0 and n == 1:
                pass_on(0, RELAY[0])
            if not final and n == PASS:
                pass_on(t + 1, RELAY[0])
            for m in LATE.get(n, ()):
                if m == 2:
                    if t == 0:
                        for array in (1, 2):
                            load_pair(array, 3).wait()
                    arrived_lev(t, LAST)
                    if t > 0:
                        sent_lev(t - 1, LAST)
                        sent_lon(t - 1, LAST)
                if m < 2:
                    arrived_lon(t, LAST, 1 - m)

                    @pl.when(wide[m])
                    def _():
                        turn_copy(t, m).wait_send()
                update_chunk(t, m)
                if not final and m < 2:
                    send_near(t + 1, m)
            if not final:
                update_planes(t, [q for q in (2 * n, 2 * n + 1) if q < EDGE])
            if final and n == 2:
                rest_1()
            if final and n == 4:
                rest_2()
        if not final:
            send_lev(t + 1, LAST)
    edge_0()
    edge_1()
    rest_3()
    edge_2()
    for n in range(CHUNKS):
        lat_copy(TICKS - CHUNKS + n).wait_send()
    for g in range(len(GROUPS)):
        sent_lev(STEPS - 1, g)
        sent_lon(STEPS - 1, g)
    for t in (STEPS - 2, STEPS - 1):
        for g in RELAY:
            for side in range(2):
                @pl.when(keeper[side])
                def _():
                    pass_copy(t, g, side).wait_send()
    prefix_end()


def finish(*refs):
    dma = pltpu.SemaphoreType.DMA
    pl.run_scoped(functools.partial(finish_with, *refs), dma((PIECES,)), dma((Q,)))


def finish_with(last, before, totals, end, run, t_sem, c_sem):
    la = lax.axis_index("lat")
    scale = 1.0 / (N * lax.axis_size("lon"))

    def place(q):
        return q + la * (Q - 1 - 2 * q)

    def put_end(p):
        planes = pl.ds(p * (Q // PIECES), Q // PIECES)
        return pltpu.make_async_copy(last.at[planes], end.at[planes], t_sem.at[p])

    def put_totals(q):
        return pltpu.make_async_copy(run.at[q], totals.at[place(q)], c_sem.at[q])

    for p in range(PIECES):
        put_end(p).start()
    for q in range(Q):
        def row(i, total):
            total = total + last[place(q), i]
            run[q, i] = total * scale
            return total
        lax.fori_loop(0, N, row, before[q])
        put_totals(q).start()
    for p in range(PIECES):
        put_end(p).wait()
    for q in range(Q):
        put_totals(q).wait()


def per_device(x, d, f):
    hbm = pl.BlockSpec(memory_space=pltpu.HBM)
    vmem = pl.BlockSpec(memory_space=pltpu.VMEM)
    slots = lax.axis_size("lon") // 2
    block = (Q, N, K, M)
    part = (Q, K, M)
    f32 = jnp.float32
    last, before = pl.pallas_call(
        exchange,
        out_shape=(pltpu.VMEM(block, f32), pltpu.VMEM(part, f32)),
        in_specs=[hbm] * 3,
        out_specs=(vmem, vmem),
        scratch_shapes=[
            pltpu.VMEM((2, Q + 2, N + 2, K + 2 * PAD, M), f32),
            pltpu.VMEM(block, f32),
            pltpu.VMEM(block, f32),
            pltpu.VMEM((STEPS, len(RELAY), 3, K, M), f32),
            pltpu.VMEM(part, f32),
            pltpu.VMEM(part, f32),
            pltpu.VMEM((EDGE, K, M), f32),
            pltpu.VMEM((K, M), f32),
            pltpu.VMEM((EDGE, K, M), f32),
            pltpu.VMEM((EDGE, K, M), f32),
            pltpu.VMEM((EDGE, K, M), f32),
            pltpu.VMEM((slots - 1, K, M), f32),
        ],
        compiler_params=pltpu.CompilerParams(
            collective_id=0, has_side_effects=True, vmem_limit_bytes=52 * 1024 * 1024),
        name="exchange",
    )(x, d, f)
    totals, end = pl.pallas_call(
        finish,
        out_shape=(jax.ShapeDtypeStruct(block, f32), jax.ShapeDtypeStruct(block, f32)),
        in_specs=[vmem, vmem],
        out_specs=(hbm, hbm),
        scratch_shapes=[pltpu.VMEM(block, f32)],
        compiler_params=pltpu.CompilerParams(vmem_limit_bytes=16 * 1024 * 1024),
        name="finish",
    )(last, before)
    return totals, end


def solution(mesh):
    spec = P("lat", "lon", "lev", None)
    return jax.shard_map(
        per_device, mesh=mesh, in_specs=(spec,) * 3, out_specs=(spec, spec), check_vma=False)
```

```python
import functools

import jax
import jax.numpy as jnp
from jax import lax
from jax.experimental import pallas as pl
from jax.experimental.pallas import tpu as pltpu
from jax.sharding import PartitionSpec as P

STEPS = 4
MESH = pl.DeviceIdType.MESH
Q, N, K, M = 8, 32, 64, 128
PAD = 8
TOP = PAD + K
EDGE = Q - 1
CHUNKS = 8
ROWS = N // CHUNKS
ORDER = (0, 7, 1, 2, 3, 4, 5, 6)
WINDOW = 5
TICKS = STEPS * CHUNKS
GROUPS = ((0, 4), (4, 3), (7, 1))
LAST = len(GROUPS) - 1
RELAY = ((1, 1), (0, 1), (0, 1), (1, 1))
LATE = {2: (2, 0), 3: (3, 1), 4: (4,), 5: (5,), 6: (6,), 7: (7,)}
PIECES = 4
A, B = 0, 1
PASS = 5
PLANES = ((0, Q - 1), (Q - 1, 1))
GREET = ((6, (1,)), (5, (1,)), (3, (0, 1, 3, 4)), (1, range(7)), (2, (0, 1, 3, 4, 5)), (4, (0, 1, 2, 3)))


def exchange(*refs):
    dma = pltpu.SemaphoreType.DMA
    groups, slots = len(GROUPS), lax.axis_size("lon") // 2
    own = (dma((Q,)), dma((2, Q // 2)), dma((TICKS,)), dma((2, groups, 2)), dma((2, groups, 2)),
           dma((2,)), dma, dma((2,)), dma, dma, dma, dma((slots - 1, 2)),
           dma((TICKS,)), dma((2, groups, 2)), dma((2, groups, 2)), dma((STEPS,)),
           dma((2,)), dma, dma, dma, dma((slots - 1,)))
    pl.run_scoped(functools.partial(exchange_with, refs), *own)


def exchange_with(refs, in_sem, pair_sem, lat_s, lon_s, lev_s, hold_s, turn_s, mate_s, z_s, x_s, back_s, far_s,
                  lat_r, lon_r, lev_r, hold_r, mate_r, z_r, x_r, back_r, far_r):
    (x, d, f, last, before, s, dv, fv, hold, tot, mate, pair, joint, over_z, over_x, through, earlier) = refs
    la, lo, le = lax.axis_index("lat"), lax.axis_index("lon"), lax.axis_index("lev")
    lon_size, lev_size = lax.axis_size("lon"), lax.axis_size("lev")
    half = lon_size // 2
    has_lon = (lo > 0, lo < lon_size - 1)
    has_lev = (le > 0, le < lev_size - 1)
    odd = lo % 2 == 1
    even = lo % 2 == 0
    near = (odd, even)
    wide = (even & (lo > 0), odd & (lo < lon_size - 1))
    slots = lon_size // 2
    cells = pl.ds(PAD, K)

    def place(q):
        return q + la * (Q - 1 - 2 * q)

    def load(q):
        return pltpu.make_async_copy(x.at[place(q)], s.at[0, q + 1, pl.ds(1, N), cells, :], in_sem.at[q])

    def load_pair(n, p):
        planes = pl.ds(2 * p + la * (Q - 2 - 4 * p), 2)
        return pltpu.make_async_copy((d, f)[n - 1].at[planes], (dv, fv)[n - 1].at[planes], pair_sem.at[n - 1, p])

    load(EDGE).start()

    barrier = pltpu.get_barrier_semaphore()

    def greet(dev):
        pl.semaphore_signal(barrier, inc=1, device_id=dev, device_id_type=MESH)

    def among(members):
        found = lo < 0
        for m in members:
            found = found | (lo == m)
        return found

    count = jnp.int32(1)
    peers = [
        (has_lev[0], (la, lo, le - 1)),
        (has_lev[1], (la, lo, le + 1)),
    ]
    for offset, lower in GREET:
        peers.append((among(lower), (la, lo + offset, le)))
        peers.append((among([m + offset for m in lower]), (la, lo - offset, le)))
    peers += [
        (wide[0], (1 - la, lo - 1, le)),
        (wide[1], (1 - la, lo + 1, le)),
    ]
    for there, dev in peers:
        count = count + there.astype(jnp.int32)

        @pl.when(there)
        def _():
            greet(dev)

    greet((1 - la, lo, le))
    for q in range(EDGE):
        load(q).start()
    pl.semaphore_wait(barrier, count)

    zero_row = jnp.zeros((K, M), jnp.float32)
    zero_cell = jnp.zeros((1, M), jnp.float32)

    def lat_copy(tick):
        t, c = tick // CHUNKS, ORDER[tick % CHUNKS]
        rows = pl.ds(1 + c * ROWS, ROWS)
        return pltpu.make_async_remote_copy(
            src_ref=s.at[t % 2, Q, rows, cells, :],
            dst_ref=s.at[t % 2, Q + 1, rows, cells, :],
            send_sem=lat_s.at[tick], recv_sem=lat_r.at[tick],
            device_id=(1 - la, lo, le), device_id_type=MESH)

    FROM, TO = (1, N), (N + 1, 0)

    def face(t, g, i):
        q, n = GROUPS[g]
        return s.at[t % 2, pl.ds(q + 1, n), i, cells, :]

    def lon_copy(t, g, side):
        return pltpu.make_async_remote_copy(
            src_ref=face(t, g, FROM[side]), dst_ref=face(t, g, TO[side]),
            send_sem=lon_s.at[t % 2, g, side], recv_sem=lon_r.at[t % 2, g, side],
            device_id=(la, lo + (-1, 1)[side], le), device_id_type=MESH)

    def hold_copy(t, side):
        g = RELAY[t][side]
        return pltpu.make_async_remote_copy(
            src_ref=face(t, g, FROM[side]), dst_ref=hold.at[t, pl.ds(0, GROUPS[g][1])],
            send_sem=lon_s.at[t % 2, g, side], recv_sem=hold_r.at[t],
            device_id=(la, lo + (-half, half)[side], le), device_id_type=MESH)

    def pass_copy(t, side):
        g = RELAY[t][side]
        return pltpu.make_async_remote_copy(
            src_ref=hold.at[t, pl.ds(0, GROUPS[g][1])], dst_ref=face(t, g, TO[side]),
            send_sem=hold_s.at[t % 2], recv_sem=lon_r.at[t % 2, g, side],
            device_id=(la, lo + (half - 1, 1 - half)[side], le), device_id_type=MESH)

    def turn_copy(t, side):
        return pltpu.make_async_remote_copy(
            src_ref=s.at[t % 2, Q + 1, FROM[side], cells, :],
            dst_ref=s.at[t % 2, Q, TO[side], cells, :],
            send_sem=turn_s, recv_sem=lon_r.at[t % 2, LAST, side],
            device_id=(1 - la, lo + (-1, 1)[side], le), device_id_type=MESH)

    def lev_copy(t, g, side):
        q, n = GROUPS[g]
        planes = pl.ds(q + 1, n)
        return pltpu.make_async_remote_copy(
            src_ref=s.at[t % 2, planes, pl.ds(1, N), pl.ds((PAD, TOP - 1)[side], 1), :],
            dst_ref=s.at[t % 2, planes, pl.ds(1, N), pl.ds((TOP, PAD - 1)[side], 1), :],
            send_sem=lev_s.at[t % 2, g, side], recv_sem=lev_r.at[t % 2, g, side],
            device_id=(la, lo, le + (-1, 1)[side]), device_id_type=MESH)

    sender = (lo == half, lo == half - 1)
    keeper = (lo == 0, lo == lon_size - 1)

    def send_lev(t, q):
        for side in range(2):
            @pl.when(has_lev[side])
            def _():
                lev_copy(t, q, side).start()

    def send_lon(t, q):
        for side in range(2):
            if q == RELAY[t][side]:
                @pl.when(has_lon[side] & jnp.logical_not(sender[side]))
                def _():
                    lon_copy(t, q, side).start()

                @pl.when(sender[side])
                def _():
                    hold_copy(t, side).start()
            else:
                @pl.when(has_lon[side])
                def _():
                    lon_copy(t, q, side).start()

    def send_near(t, side):
        @pl.when(near[side])
        def _():
            lon_copy(t, LAST, side).start()

    def pass_on(t):
        for side in range(2):
            @pl.when(keeper[side])
            def _():
                if t > 1:
                    pass_copy(t - 2, side).wait_send()
                hold_copy(t, side).wait_recv()
                pass_copy(t, side).start()

    def sent_lev(t, q):
        for side in range(2):
            @pl.when(has_lev[side])
            def _():
                lev_copy(t, q, side).wait_send()

    def sent_lon(t, q):
        for side in range(2):
            @pl.when(near[side] if q == LAST else has_lon[side])
            def _():
                lon_copy(t, q, side).wait_send()

    def arrived_lev(t, q):
        for side in range(2):
            @pl.when(has_lev[1 - side])
            def _():
                lev_copy(t, q, side).wait_recv()

    def arrived_lon(t, q, side):
        @pl.when(has_lon[1 - side])
        def _():
            lon_copy(t, q, side).wait_recv()

    def update(t, q, i):
        b = t % 2
        here = s.at[b, q + 1, i + 1]
        middle = here[cells, :]
        spread = here[pl.ds(PAD - 1, K), :] + here[pl.ds(PAD + 1, K), :]
        spread += s[b, q + 1, i, cells, :] + s[b, q + 1, i + 2, cells, :]
        spread += s[b, q, i + 1, cells, :] + s[b, q + 2, i + 1, cells, :]
        j = place(q)
        new = middle + dv[j, i] * (spread - 6.0 * middle) + fv[j, i]
        if t == STEPS - 1:
            last[j, i] = new
        else:
            s[1 - b, q + 1, i + 1, cells, :] = new
        return new

    def update_plane(t, q):
        if t == STEPS - 1:
            def add(i, total):
                return total + update(t, q, i)
            tot[q] = lax.fori_loop(0, N, add, zero_row)
        else:
            @pl.loop(0, N)
            def _(i):
                update(t, q, i)

    def update_chunk(t, n):
        c = ORDER[n]
        if t == STEPS - 1:
            def add(i, total):
                return total + update(t, EDGE, i)
            total = lax.fori_loop(c * ROWS, (c + 1) * ROWS, add, zero_row)
            if n == LATE[2][0]:
                tot[EDGE] = total
            else:
                tot[EDGE] = tot[EDGE] + total
        else:
            @pl.loop(c * ROWS, (c + 1) * ROWS)
            def _(i):
                update(t, EDGE, i)

    def mate_copy(group):
        planes = pl.ds(*PLANES[group])
        return pltpu.make_async_remote_copy(
            src_ref=tot.at[planes], dst_ref=mate.at[planes],
            send_sem=mate_s.at[group], recv_sem=mate_r.at[group],
            device_id=(la, lo + (-1, 1)[group], le), device_id_type=MESH)

    rest = pl.ds(*PLANES[A])

    def z_copy():
        return pltpu.make_async_remote_copy(
            src_ref=pair, dst_ref=over_z, send_sem=z_s, recv_sem=z_r,
            device_id=(la, lo + half, le), device_id_type=MESH)

    def x_copy(source, offset):
        return pltpu.make_async_remote_copy(
            src_ref=source, dst_ref=over_x, send_sem=x_s, recv_sem=x_r,
            device_id=(la, lo + offset, le), device_id_type=MESH)

    def back_copy():
        return pltpu.make_async_remote_copy(
            src_ref=through, dst_ref=before.at[rest], send_sem=back_s, recv_sem=back_r,
            device_id=(la, lo + 1, le), device_id_type=MESH)

    def far_copy(far, to_odd):
        return pltpu.make_async_remote_copy(
            src_ref=joint, dst_ref=earlier.at[far - 1],
            send_sem=far_s.at[far - 1, to_odd], recv_sem=far_r.at[far - 1],
            device_id=(la, lo + 2 * far - 1 + to_odd, le), device_id_type=MESH)

    low_even = even & (lo < half)

    def rest_0():
        @pl.when(odd)
        def _():
            mate_copy(A).start()

    def rest_1():
        @pl.when(even)
        def _():
            mate_copy(A).wait_recv()

            @pl.loop(0, EDGE)
            def _(q):
                pair[q] = tot[q] + mate[q]

        @pl.when(lo == 0)
        def _():
            x_copy(pair, 2).start()

        @pl.when(low_even)
        def _():
            z_copy().start()

    def rest_2():
        @pl.when(lo == half)
        def _():
            z_copy().wait_recv()

            @pl.loop(0, EDGE)
            def _(q):
                pair[q] = pair[q] + over_z[q]

            x_copy(pair, 2).start()

        @pl.when(lo == half + 2)
        def _():
            z_copy().wait_recv()
            x_copy(over_z, -2).start()

    def rest_3():
        @pl.when(even & (lo > 0))
        def _():
            x_copy(pair, 2).wait_recv()

        @pl.when(lo == 0)
        def _():
            @pl.loop(0, EDGE)
            def _(q):
                before[q] = zero_row

        @pl.when(even & (lo > 0))
        def _():
            @pl.loop(0, EDGE)
            def _(q):
                before[q] = over_x[q]

        @pl.when(even & (lo >= half))
        def _():
            @pl.loop(0, EDGE)
            def _(q):
                before[q] = before[q] + over_z[q]

        @pl.when(even)
        def _():
            @pl.loop(0, EDGE)
            def _(q):
                through[q] = before[q] + tot[q]

            back_copy().start()

    def edge_0():
        @pl.when(even)
        def _():
            mate_copy(B).start()

    FARS = (3, 1, 2)

    def edge_1():
        @pl.when(odd)
        def _():
            mate_copy(B).wait_recv()
            joint[...] = tot[EDGE] + mate[EDGE]
            for far in FARS:
                @pl.when(lo + 2 * far < lon_size)
                def _():
                    for to_odd in ((0, 1) if far == 1 else (1, 0)):
                        far_copy(far, to_odd).start()

    def edge_2():
        before[EDGE] = zero_row
        for far in range(1, slots):
            @pl.when(lo >= 2 * far)
            def _():
                far_copy(far, 1).wait_recv()
                before[EDGE] = before[EDGE] + earlier[far - 1]

        @pl.when(odd)
        def _():
            before[EDGE] = before[EDGE] + mate[EDGE]

    def prefix_end():
        @pl.when(odd)
        def _():
            back_copy().wait_recv()
            mate_copy(A).wait_send()
            for far in FARS:
                @pl.when(lo + 2 * far < lon_size)
                def _():
                    far_copy(far, 1).wait_send()
                    far_copy(far, 0).wait_send()

        @pl.when(even)
        def _():
            back_copy().wait_send()
            mate_copy(B).wait_send()

        @pl.when(low_even)
        def _():
            z_copy().wait_send()

        @pl.when(among((0, half, half + 2)))
        def _():
            x_copy(pair, 2).wait_send()

    def send_lat(tick):
        if tick >= CHUNKS:
            lat_copy(tick - CHUNKS).wait_send()
        lat_copy(tick).start()

    load(EDGE).wait()
    send_lat(0)
    send_lat(1)
    for p in (0, 3, 1, 2):
        load_pair(1, p).start()
        load_pair(2, p).start()
    send_lev(0, LAST)
    for side in range(2):
        send_near(0, side)

    @pl.loop(0, N)
    def _(i):
        for b in range(2):
            s[b, 0, i + 1, cells, :] = zero_row

    for side, row in ((0, 0), (1, N + 1)):
        @pl.when(jnp.logical_not(has_lon[side]))
        def _():
            @pl.loop(0, Q)
            def _(q):
                for b in range(2):
                    s[b, q + 1, row, cells, :] = zero_row

    for side, cell in ((0, PAD - 1), (1, TOP)):
        @pl.when(jnp.logical_not(has_lev[side]))
        def _():
            @pl.loop(0, Q)
            def _(q):
                @pl.loop(0, N)
                def _(i):
                    for b in range(2):
                        s[b, q + 1, i + 1, pl.ds(cell, 1), :] = zero_cell

    for g in range(LAST):
        q0, planes = GROUPS[g]
        for q in range(q0, q0 + planes):
            load(q).wait()
        send_lev(0, g)
        send_lon(0, g)
        send_lat(g + 2)
    for tick in range(4, WINDOW):
        send_lat(tick)

    def update_planes(t, planes):
        for q in planes:
            g = q // 4
            q0, n = GROUPS[g]
            if t == 0 and q % 2 == 0 and q // 2 < 3:
                for array in (1, 2):
                    load_pair(array, q // 2).wait()
            if q == q0:
                arrived_lev(t, g)
                for side in range(2):
                    arrived_lon(t, g, side)
                if t > 0:
                    sent_lev(t - 1, g)
                    sent_lon(t - 1, g)
            update_plane(t, q)
            if t < STEPS - 1 and q == q0 + n - 1:
                send_lev(t + 1, g)
                send_lon(t + 1, g)

    for t in range(STEPS):
        final = t == STEPS - 1
        for n in range(CHUNKS):
            tick = t * CHUNKS + n
            if final and n == 0:
                update_planes(t, range(EDGE))
                rest_0()
            lat_copy(tick).wait_recv()
            if tick + WINDOW < TICKS:
                send_lat(tick + WINDOW)
            if n < 2:
                @pl.when(wide[n])
                def _():
                    turn_copy(t, n).start()
            if t == 0 and n == 1:
                pass_on(0)
            if not final and n == PASS:
                pass_on(t + 1)
            for m in LATE.get(n, ()):
                if m == 2:
                    if t == 0:
                        for array in (1, 2):
                            load_pair(array, 3).wait()
                    arrived_lev(t, LAST)
                    if t > 0:
                        sent_lev(t - 1, LAST)
                        sent_lon(t - 1, LAST)
                if m < 2:
                    arrived_lon(t, LAST, 1 - m)

                    @pl.when(wide[m])
                    def _():
                        turn_copy(t, m).wait_send()
                update_chunk(t, m)
                if not final and m < 2:
                    send_near(t + 1, m)
            if not final:
                update_planes(t, [q for q in (2 * n, 2 * n + 1) if q < EDGE])
            if final and n == 2:
                rest_1()
            if final and n == 4:
                rest_2()
        if not final:
            send_lev(t + 1, LAST)
    edge_0()
    edge_1()
    rest_3()
    edge_2()
    for n in range(CHUNKS):
        lat_copy(TICKS - CHUNKS + n).wait_send()
    for g in range(len(GROUPS)):
        sent_lev(STEPS - 1, g)
        sent_lon(STEPS - 1, g)
    for t in (STEPS - 2, STEPS - 1):
        for side in range(2):
            @pl.when(keeper[side])
            def _():
                pass_copy(t, side).wait_send()
    prefix_end()


def finish(*refs):
    dma = pltpu.SemaphoreType.DMA
    pl.run_scoped(functools.partial(finish_with, *refs), dma((PIECES,)), dma((Q,)))


def finish_with(last, before, totals, end, run, t_sem, c_sem):
    la = lax.axis_index("lat")
    scale = 1.0 / (N * lax.axis_size("lon"))

    def place(q):
        return q + la * (Q - 1 - 2 * q)

    def put_end(p):
        planes = pl.ds(p * (Q // PIECES), Q // PIECES)
        return pltpu.make_async_copy(last.at[planes], end.at[planes], t_sem.at[p])

    def put_totals(q):
        return pltpu.make_async_copy(run.at[q], totals.at[place(q)], c_sem.at[q])

    for p in range(PIECES):
        put_end(p).start()
    for q in range(Q):
        def row(i, total):
            total = total + last[place(q), i]
            run[q, i] = total * scale
            return total
        lax.fori_loop(0, N, row, before[q])
        put_totals(q).start()
    for p in range(PIECES):
        put_end(p).wait()
    for q in range(Q):
        put_totals(q).wait()


def per_device(x, d, f):
    hbm = pl.BlockSpec(memory_space=pltpu.HBM)
    vmem = pl.BlockSpec(memory_space=pltpu.VMEM)
    slots = lax.axis_size("lon") // 2
    block = (Q, N, K, M)
    part = (Q, K, M)
    f32 = jnp.float32
    last, before = pl.pallas_call(
        exchange,
        out_shape=(pltpu.VMEM(block, f32), pltpu.VMEM(part, f32)),
        in_specs=[hbm] * 3,
        out_specs=(vmem, vmem),
        scratch_shapes=[
            pltpu.VMEM((2, Q + 2, N + 2, K + 2 * PAD, M), f32),
            pltpu.VMEM(block, f32),
            pltpu.VMEM(block, f32),
            pltpu.VMEM((STEPS, 4, K, M), f32),
            pltpu.VMEM(part, f32),
            pltpu.VMEM(part, f32),
            pltpu.VMEM((EDGE, K, M), f32),
            pltpu.VMEM((K, M), f32),
            pltpu.VMEM((EDGE, K, M), f32),
            pltpu.VMEM((EDGE, K, M), f32),
            pltpu.VMEM((EDGE, K, M), f32),
            pltpu.VMEM((slots - 1, K, M), f32),
        ],
        compiler_params=pltpu.CompilerParams(
            collective_id=0, has_side_effects=True, vmem_limit_bytes=52 * 1024 * 1024),
        name="exchange",
    )(x, d, f)
    totals, end = pl.pallas_call(
        finish,
        out_shape=(jax.ShapeDtypeStruct(block, f32), jax.ShapeDtypeStruct(block, f32)),
        in_specs=[vmem, vmem],
        out_specs=(hbm, hbm),
        scratch_shapes=[pltpu.VMEM(block, f32)],
        compiler_params=pltpu.CompilerParams(vmem_limit_bytes=16 * 1024 * 1024),
        name="finish",
    )(last, before)
    return totals, end


def solution(mesh):
    spec = P("lat", "lon", "lev", None)
    return jax.shard_map(
        per_device, mesh=mesh, in_specs=(spec,) * 3, out_specs=(spec, spec), check_vma=False)
```
